128 devices in a mesh: peer: 32 (over z_hi, x, y), zero: 4 (over z_lo, core).
Axes of the slice: x: 4, y: 4, z: 4 (z_hi: 2, z_lo: 2; z = z_hi * 2 + z_lo), core: 2. Of those that a mesh axis runs over, the one named last changes fastest.
Arguments:
- tokens: bfloat16 [32, 2048, 1024], P('peer', 'zero'), may hold values from -6 to 6
- out_grad: bfloat16 [32, 2048, 1024], P('peer', 'zero'), may hold values from -6 to 6
- step: int32 [1], replicated, may hold values from 0 to 3999
- up_param: float32 [32, 1024, 2048], P('peer', 'zero'), may hold values from -0.2 to 0.2
- down_param: float32 [32, 2048, 1024], P('peer', 'zero'), may hold values from -0.2 to 0.2
- up_first: float32 [32, 1024, 2048], P('peer', 'zero'), may hold values from -27.1529 to 27.1529
- down_first: float32 [32, 2048, 1024], P('peer', 'zero'), may hold values from -27.1529 to 27.1529
- up_second: float32 [32, 1024, 2048], P('peer', 'zero'), may hold values from 0.8192 to 819.2
- down_second: float32 [32, 2048, 1024], P('peer', 'zero'), may hold values from 0.8192 to 819.2
Outputs:
- new_up: float32 [32, 1024, 2048], P('peer', 'zero')
- new_down: float32 [32, 2048, 1024], P('peer', 'zero')
- new_up_first: float32 [32, 1024, 2048], P('peer', 'zero')
- new_down_first: float32 [32, 2048, 1024], P('peer', 'zero')
- new_up_second: float32 [32, 1024, 2048], P('peer', 'zero')
- new_down_second: float32 [32, 2048, 1024], P('peer', 'zero')
The draws below stay inside these ranges and needn't reach their ends.
All inputs are finite; a program needn't handle non-finite values.
Results may differ from the reference program's by a relative error of at most 0.0065.
Values may be sent and summed in bfloat16 or wider, within the bound.
A program may use at most 128 MiB of HBM per device.

```python
import math
import jax
import jax.numpy as jnp
from jax import lax

D = 1024
FFW = 2048
GTOK = 2048
GROUPS = 32
N_PEER = 32


def block_levels(key, shape, cuts, low, high):
    level = 1.0
    for position, blocks in cuts:
        steps = jax.random.uniform(jax.random.fold_in(jax.random.fold_in(key, 6), position), (blocks,), jnp.float32, low / len(cuts), high / len(cuts))
        level = level * jnp.repeat(jnp.exp(steps), shape[position] // blocks).reshape((-1,) + (1,) * (len(shape) - 1 - position))
    return level


def scatter_about(own_key, shape, width, limit, pieces=(), held_as=jnp.bfloat16):
    values = width * jax.random.normal(own_key, shape, jnp.float32)
    if pieces:
        values = values * block_levels(own_key, shape, pieces, -0.22, 0.18)
    return jnp.clip(values, -limit, limit).astype(held_as)


def setup_inputs(seed: int = 0) -> dict:
    splits = jax.random.split(jax.random.key(seed), 10)
    tokens = scatter_about(splits[0], (GROUPS, GTOK, D), 1.0, 6.0, ((0, 32), (1, 4)))
    out_grad = scatter_about(splits[1], (GROUPS, GTOK, D), 1.0, 6.0, ((0, 32), (1, 4)))
    step = jax.random.randint(splits[2], (1,), 0, 4000).astype(jnp.int32)
    up_param = scatter_about(splits[3], (GROUPS, D, FFW), 0.03, 0.2, ((0, 32), (1, 4)), jnp.float32)
    down_param = scatter_about(splits[4], (GROUPS, FFW, D), 0.03, 0.2, ((0, 32), (1, 4)), jnp.float32)
    up_first = scatter_about(splits[5], (GROUPS, D, FFW), (0.1 * GTOK ** 0.5), 27.1529, ((0, 32), (1, 4)), jnp.float32)
    down_first = scatter_about(splits[6], (GROUPS, FFW, D), (0.1 * GTOK ** 0.5), 27.1529, ((0, 32), (1, 4)), jnp.float32)
    up_second = jnp.clip(jnp.exp(math.log(819.2) - 6.9077553 * jax.random.uniform(splits[7], (GROUPS, D, FFW), jnp.float32) ** block_levels(splits[7], (GROUPS, D, FFW), ((0, 32), (1, 4)), -0.2, 0.2)), 0.8192, 819.2)
    down_second = jnp.clip(jnp.exp(math.log(819.2) - 6.9077553 * jax.random.uniform(splits[8], (GROUPS, FFW, D), jnp.float32) ** block_levels(splits[8], (GROUPS, FFW, D), ((0, 32), (1, 4)), -0.2, 0.2)), 0.8192, 819.2)
    return {"tokens": tokens, "out_grad": out_grad, "step": step, "up_param": up_param, "down_param": down_param, "up_first": up_first, "down_first": down_first, "up_second": up_second, "down_second": down_second}


def gelu_tanh(values):
    return 0.5 * values * (1.0 + jnp.tanh(0.7978845608 * (values + 0.044715 * values * values * values)))

def group_grads(items):
    tokens, out_grad, up_param, down_param = items
    widened = tokens.astype(jnp.float32)
    center = lax.optimization_barrier(jnp.mean(widened, axis=1, keepdims=True))
    spread = lax.optimization_barrier(jnp.mean((widened - center) * (widened - center), axis=1, keepdims=True))
    normed = ((widened - center) * lax.rsqrt(spread + 1e-05)).astype(jnp.bfloat16)
    up_low = up_param.astype(jnp.bfloat16)
    down_low = down_param.astype(jnp.bfloat16)
    pre = jnp.dot(normed, up_low, preferred_element_type=jnp.float32)
    active, backward = jax.vjp(gelu_tanh, pre)
    act = active.astype(jnp.bfloat16)
    act_grad = jnp.dot(out_grad, down_low.T, preferred_element_type=jnp.float32)
    pre_grad = backward(act_grad)[0].astype(jnp.bfloat16)
    up_grad = jnp.dot(normed.T, pre_grad, preferred_element_type=jnp.float32)
    down_grad = jnp.dot(act.T, out_grad, preferred_element_type=jnp.float32)
    return (up_grad, down_grad)

def adam_update(param, first, second, grad, first_fix, second_fix):
    first_new = 0.9 * first + 0.1 * grad
    second_new = 0.999 * second + 0.001 * grad * grad
    local = param - 0.01 * (first_new / first_fix) / (jnp.sqrt(second_new / second_fix) + 1e-08)
    return (local, first_new, second_new)

def reference(tokens, out_grad, step, up_param, down_param, up_first, down_first, up_second, down_second):
    up_grad, down_grad = lax.map(group_grads, (tokens, out_grad, up_param, down_param))
    count = (step[0] + 1).astype(jnp.float32)
    first_fix = 1.0 - jnp.power(jnp.float32(0.9), count)
    second_fix = 1.0 - jnp.power(jnp.float32(0.999), count)
    up_local, up_first_new, up_second_new = adam_update(up_param, up_first, up_second, up_grad, first_fix, second_fix)
    down_local, down_first_new, down_second_new = adam_update(down_param, down_first, down_second, down_grad, first_fix, second_fix)
    levels = N_PEER.bit_length() - 1
    distance = jnp.left_shift(jnp.int32(1), (step[0] % levels).astype(jnp.int32))
    partner = ((jnp.arange(N_PEER, dtype=jnp.int32) + distance) % N_PEER).astype(jnp.int32)
    new_up = 0.5 * (up_local + jnp.take(up_local, partner, axis=0))
    new_down = 0.5 * (down_local + jnp.take(down_local, partner, axis=0))
    return (new_up, new_down, up_first_new, down_first_new, up_second_new, down_second_new)
```

```python
from functools import partial

import jax
import jax.numpy as jnp
from jax import lax
from jax.experimental import pallas as pl
from jax.experimental.pallas import tpu as pltpu
from jax.sharding import PartitionSpec as P

MESH = pl.DeviceIdType.MESH
SLICES = 2
CHUNKS = 4
BF16 = jnp.bfloat16
F32 = jnp.float32


def dot(left, right, dims):
    return lax.dot_general(left, right, (dims, ((), ())), preferred_element_type=F32)


def kernel(
    peers,
    distance,
    fix,
    tokens,
    out_grad,
    up_param,
    down_param,
    up_first,
    down_first,
    up_second,
    down_second,
    new_up,
    new_down,
    new_up_first,
    new_down_first,
    new_up_second,
    new_down_second,
    tok,
    grd,
    nrm,
    up_p,
    up_f,
    up_s,
    dn_p,
    dn_f,
    dn_s,
    upw_send,
    upw,
    up_t,
    down_low,
    act,
    slope,
    acc_up,
    acc_down,
    ug_send,
    ug,
    dn_out,
    dn_in,
    up_out,
    up_in,
    load_sem,
    store_sem,
    far_send,
    far_recv,
    relay_send,
    relay_recv,
    near_send,
    near_recv,
    upw_ssem,
    upw_rsem,
    ug_ssem,
    ug_rsem,
    dn_ssem,
    dn_rsem,
    up_ssem,
    up_rsem,
):
    rows, width = tokens.shape
    hid = down_param.shape[0]
    part = up_param.shape[0]
    span = hid // SLICES
    piece = rows // CHUNKS
    block = 2 * piece
    own_blocks = rows // block
    blocks = tok.shape[0]
    near_blocks = 2 * own_blocks

    peer = lax.axis_index("peer")
    me = lax.axis_index("zero")
    mate = me + 1 - 2 * (me % 2)
    cross = (me + 2) % 4
    diagonal = 3 - me
    group = (cross, diagonal, mate)
    onto = (peer + peers - distance) % peers
    source = (peer + distance) % peers

    def local(src, dst, sem):
        return pltpu.make_async_copy(src, dst, sem)

    def remote(src, dst, ssem, rsem, **where):
        return pltpu.make_async_remote_copy(
            src_ref=src, dst_ref=dst, send_sem=ssem, recv_sem=rsem, device_id=where, device_id_type=MESH
        )

    loads = [
        local(up_param, up_p, load_sem.at[0]),
        local(down_param, dn_p, load_sem.at[1]),
        local(down_first, dn_f, load_sem.at[2]),
        local(down_second, dn_s, load_sem.at[3]),
        local(up_first, up_f, load_sem.at[4]),
        local(up_second, up_s, load_sem.at[5]),
    ]
    for b in range(own_blocks):
        at = pl.ds(b * block, block)
        loads.append(local(tokens.at[at], tok.at[b], load_sem.at[6 + 2 * b]))
        loads.append(local(out_grad.at[at], grd.at[b], load_sem.at[7 + 2 * b]))
    loads[0].start()

    barrier = pltpu.get_barrier_semaphore()
    for other in group:
        pl.semaphore_signal(barrier, inc=1, device_id={"zero": other}, device_id_type=MESH)
    for other in (onto, source):
        pl.semaphore_signal(barrier, inc=1, device_id={"peer": other}, device_id_type=MESH)
    for copy in loads[1:]:
        copy.start()

    def far(kind, i):
        src, dst = ((tokens, tok), (out_grad, grd))[kind]
        at = pl.ds(pl.multiple_of(i * piece, piece), piece)
        return remote(
            src.at[at],
            dst.at[near_blocks + i, pl.ds(0, piece)],
            far_send.at[kind, i],
            far_recv.at[kind, i],
            zero=cross,
        )

    def relay(kind, i):
        dst = (tok, grd)[kind]
        return remote(
            dst.at[near_blocks + i, pl.ds(0, piece)],
            dst.at[near_blocks + i, pl.ds(piece, piece)],
            relay_send.at[kind, i],
            relay_recv.at[kind, i],
            zero=mate,
        )

    def near(kind, b):
        src, dst = ((tokens, tok), (out_grad, grd))[kind]
        return remote(
            src.at[pl.ds(b * block, block)],
            dst.at[own_blocks + b],
            near_send.at[kind, b],
            near_recv.at[kind, b],
            zero=mate,
        )

    def weights(s, o):
        return remote(
            upw_send.at[s, group[o]], upw.at[s, me], upw_ssem.at[s, o], upw_rsem.at[s, o], zero=group[o]
        )

    def weights_in(s, o):
        return remote(
            upw_send.at[s, group[o]], upw.at[s, group[o]], upw_ssem.at[s, o], upw_rsem.at[s, o], zero=group[o]
        )

    def grads(s, o):
        return remote(ug_send.at[s, group[o]], ug.at[s, me], ug_ssem.at[s, o], ug_rsem.at[s, o], zero=group[o])

    def grads_in(s, o):
        return remote(
            ug_send.at[s, group[o]], ug.at[s, group[o]], ug_ssem.at[s, o], ug_rsem.at[s, o], zero=group[o]
        )

    def down_away(s, h):
        at = pl.ds(h * (span // 2), span // 2)
        return remote(dn_out.at[s, at], dn_in.at[s, at], dn_ssem.at[s, h], dn_rsem.at[s, h], peer=onto)

    def up_away(s, h):
        at = pl.ds(2 * h, 2)
        return remote(up_out.at[s, at], up_in.at[s, at], up_ssem.at[s, h], up_rsem.at[s, h], peer=onto)

    pl.semaphore_wait(barrier, 5)
    far(0, 0).start()
    for kind in range(2):
        for b in range(own_blocks):
            near(kind, b).start()

    loads[0].wait()
    for s in range(SLICES):

        def lower(j, carry):
            at = pl.ds(pl.multiple_of(j * hid + s * span, span), span)
            upw_send[s, j] = up_p[:, at].astype(BF16)
            return carry

        lax.fori_loop(0, 4, lower, 0)
    for o in range(3):
        weights(0, o).start()
    far(1, 0).start()
    for i in range(1, CHUNKS):
        far(0, i).start()
        far(1, i).start()
    for s in range(1, SLICES):
        for o in range(3):
            weights(s, o).start()

    for s in range(SLICES):
        upw[s, me] = upw_send[s, me]
    loads[1].wait()

    def lower_down(r, carry):
        at = pl.ds(pl.multiple_of(r * (hid // 8), hid // 8), hid // 8)
        down_low[at] = dn_p[at].astype(BF16)
        return carry

    lax.fori_loop(0, 8, lower_down, 0)
    for copy in loads[6:]:
        copy.wait()

    def arrange(s):
        for o in range(3):
            weights_in(s, o).wait_recv()

        def turn(j, carry):
            up_t[:, pl.ds(pl.multiple_of(j * part, part), part)] = upw[s, j].astype(F32).T.astype(BF16)
            return carry

        lax.fori_loop(0, 4, turn, 0)

    def forward(b):
        pre = dot(up_t[...], nrm[b], ((1,), (1,)))
        cube = 0.044715 * pre * pre
        t = jnp.tanh(0.7978845608 * (pre + cube * pre))
        half = 0.5 * (1.0 + t)
        act[...] = (pre * half).astype(BF16)
        slope[...] = half + 0.5 * pre * (1.0 - t * t) * (0.7978845608 * (1.0 + 3.0 * cube))

    def gradients(s, b):
        act_grad = dot(down_low[pl.ds(s * span, span)], grd[b], ((1,), (1,)))
        pre_grad = (act_grad * slope[...]).astype(BF16)
        down = dot(act[...], grd[b], ((1,), (0,)))
        up = dot(pre_grad, nrm[b], ((1,), (0,)))
        acc_down[...] += down
        acc_up[...] += up

    def clear():
        acc_down[...] = jnp.zeros_like(acc_down)
        acc_up[...] = jnp.zeros_like(acc_up)

    def normalise(b):
        step = block // 4

        def some(r, carry):
            at = pl.ds(pl.multiple_of(r * step, step), step)
            wide = tok[b, at].astype(F32)
            center = jnp.mean(wide, axis=1, keepdims=True)
            wide = wide - center
            spread = jnp.mean(wide * wide, axis=1, keepdims=True)
            nrm[b, at] = (wide * lax.rsqrt(spread + 1e-05)).astype(BF16)
            return carry

        lax.fori_loop(0, 4, some, 0)

    def adam(param, first, second, grad):
        first_new = 0.9 * first + 0.1 * grad
        second_new = 0.999 * second + 0.001 * grad * grad
        step = (fix[0] * first_new) / (jnp.sqrt(second_new * fix[1]) + 1e-08)
        return param - step, first_new, second_new

    def down_update(s):
        tall = span // 4

        def some(r, carry):
            here = pl.ds(pl.multiple_of(r * tall, tall), tall)
            at = pl.ds(pl.multiple_of(s * span + r * tall, tall), tall)
            fresh = adam(dn_p[at], dn_f[at], dn_s[at], acc_down[here])
            dn_p[at], dn_f[at], dn_s[at] = fresh
            dn_out[s, here] = fresh[0].astype(BF16)
            return carry

        lax.fori_loop(0, 4, some, 0)

    def up_update(s):
        def some(j, carry):
            at = pl.ds(pl.multiple_of(j * hid + s * span, span), span)
            fresh = adam(up_p[:, at], up_f[:, at], up_s[:, at], ug[s, j].astype(F32))
            up_p[:, at], up_f[:, at], up_s[:, at] = fresh
            up_out[s, j] = fresh[0].astype(BF16)
            return carry

        lax.fori_loop(0, 4, some, 0)

    def share(s):
        def turn(j, carry):
            at = pl.ds(pl.multiple_of(j * part, part), part)
            ug_send[s, j] = acc_up[:, at].T.astype(BF16)
            return carry

        lax.fori_loop(0, 4, turn, 0)

    def down_moments(s):
        at = pl.ds(s * span, span)
        return (
            local(dn_f.at[at], new_down_first.at[at], store_sem.at[4 * s]),
            local(dn_s.at[at], new_down_second.at[at], store_sem.at[4 * s + 1]),
        )

    clear()
    arrange(0)

    def first_pass(b, carry):
        i = jnp.maximum(b - near_blocks, 0)

        @pl.when(jnp.logical_and(b >= own_blocks, b < near_blocks))
        def _():
            remote_near(0, b).wait_recv()

        @pl.when(b >= near_blocks)
        def _():
            far(0, i).wait_recv()
            relay(0, i).start()
            relay(0, i).wait_recv()

        normalise(b)
        forward(b)

        @pl.when(jnp.logical_and(b >= own_blocks, b < near_blocks))
        def _():
            remote_near(1, b).wait_recv()

        @pl.when(b >= near_blocks)
        def _():
            far(1, i).wait_recv()
            relay(1, i).start()
            relay(1, i).wait_recv()

        gradients(0, b)
        return carry

    def remote_near(kind, b):
        src, dst = ((tokens, tok), (out_grad, grd))[kind]
        n = jnp.clip(b - own_blocks, 0, own_blocks - 1)
        return remote(
            src.at[pl.ds(pl.multiple_of(n * block, block), block)],
            dst.at[own_blocks + n],
            near_send.at[kind, n],
            near_recv.at[kind, n],
            zero=mate,
        )

    lax.fori_loop(0, blocks, first_pass, 0)

    for copy in loads[2:6]:
        copy.wait()
    down_update(0)
    share(0)
    for h in range(2):
        down_away(0, h).start()
    for copy in down_moments(0):
        copy.start()
    ug[0, me] = ug_send[0, me]
    for o in range(3):
        grads(0, o).start()

    clear()
    arrange(1)

    def second_pass(b, carry):
        @pl.when(b == blocks // 2)
        def _():
            for o in range(3):
                grads_in(0, o).wait_recv()
            up_update(0)
            for h in range(2):
                up_away(0, h).start()

        forward(b)
        gradients(1, b)
        return carry

    lax.fori_loop(0, blocks, second_pass, 0)
    share(1)
    down_update(1)
    for o in range(3):
        grads(1, o).start()
    ug[1, me] = ug_send[1, me]
    for h in range(2):
        down_away(1, h).start()
    for copy in down_moments(1):
        copy.start()

    def down_mean(s, h):
        here = pl.ds(h * (span // 2), span // 2)
        at = pl.ds(s * span + h * (span // 2), span // 2)
        down_away(s, h).wait_recv()
        dn_p[at] = 0.5 * (dn_p[at] + dn_in[s, here].astype(F32))
        local(dn_p.at[at], new_down.at[at], store_sem.at[8 + 2 * s + h]).start()

    def up_mean_copy(s, j):
        at = pl.ds(j * hid + s * span, span)
        return local(up_p.at[:, at], new_up.at[:, at], store_sem.at[12 + 4 * s + j])

    def up_mean(s, h):
        up_away(s, h).wait_recv()
        for j in (2 * h, 2 * h + 1):
            at = pl.ds(j * hid + s * span, span)
            up_p[:, at] = 0.5 * (up_p[:, at] + up_in[s, j].astype(F32))
            up_mean_copy(s, j).start()

    for h in range(2):
        down_mean(0, h)
    for o in range(3):
        grads_in(1, o).wait_recv()
    up_update(1)
    for h in range(2):
        up_away(1, h).start()
    up_moments = (
        local(up_f, new_up_first, store_sem.at[2]),
        local(up_s, new_up_second, store_sem.at[3]),
    )
    for copy in up_moments:
        copy.start()
    for h in range(2):
        up_mean(0, h)
    for h in range(2):
        down_mean(1, h)
    for h in range(2):
        up_mean(1, h)

    for kind in range(2):
        for i in range(CHUNKS):
            far(kind, i).wait_send()
            relay(kind, i).wait_send()
        for b in range(own_blocks):
            near(kind, b).wait_send()
    for s in range(SLICES):
        for o in range(3):
            weights(s, o).wait_send()
            grads(s, o).wait_send()
        for h in range(2):
            down_away(s, h).wait_send()
            up_away(s, h).wait_send()
        for copy in down_moments(s):
            copy.wait()
        for h in range(2):
            at = pl.ds(s * span + h * (span // 2), span // 2)
            local(dn_p.at[at], new_down.at[at], store_sem.at[8 + 2 * s + h]).wait()
        for j in range(4):
            up_mean_copy(s, j).wait()
    for copy in up_moments:
        copy.wait()


def fused(level, peers, fix, *arrays):
    tokens, out_grad, up_param, down_param = arrays[:4]
    rows, width = tokens.shape
    hid = down_param.shape[0]
    part, full = up_param.shape
    span = hid // SLICES
    piece = rows // CHUNKS
    block = 2 * piece
    blocks = 4 * rows // block
    own_blocks = rows // block
    dma = pltpu.SemaphoreType.DMA
    vmem = pltpu.VMEM
    shapes = [
        jax.ShapeDtypeStruct(up_param.shape, F32),
        jax.ShapeDtypeStruct(down_param.shape, F32),
    ] * 3
    return pl.pallas_call(
        partial(kernel, peers, 2**level),
        out_shape=shapes,
        in_specs=[pl.BlockSpec(memory_space=pltpu.SMEM)] + [pl.BlockSpec(memory_space=pl.ANY)] * 8,
        out_specs=[pl.BlockSpec(memory_space=pl.ANY)] * 6,
        scratch_shapes=[
            vmem((blocks, block, width), BF16),
            vmem((blocks, block, width), BF16),
            vmem((blocks, block, width), BF16),
            vmem((part, full), F32),
            vmem((part, full), F32),
            vmem((part, full), F32),
            vmem((hid, width), F32),
            vmem((hid, width), F32),
            vmem((hid, width), F32),
            vmem((SLICES, 4, part, span), BF16),
            vmem((SLICES, 4, part, span), BF16),
            vmem((span, width), BF16),
            vmem((hid, width), BF16),
            vmem((span, block), BF16),
            vmem((span, block), F32),
            vmem((span, width), F32),
            vmem((span, width), F32),
            vmem((SLICES, 4, part, span), BF16),
            vmem((SLICES, 4, part, span), BF16),
            vmem((SLICES, span, width), BF16),
            vmem((SLICES, span, width), BF16),
            vmem((SLICES, 4, part, span), BF16),
            vmem((SLICES, 4, part, span), BF16),
            dma((6 + 2 * own_blocks,)),
            dma((12 + 4 * SLICES,)),
            dma((2, CHUNKS)),
            dma((2, CHUNKS)),
            dma((2, CHUNKS)),
            dma((2, CHUNKS)),
            dma((2, own_blocks)),
            dma((2, own_blocks)),
            dma((SLICES, 3)),
            dma((SLICES, 3)),
            dma((SLICES, 3)),
            dma((SLICES, 3)),
            dma((SLICES, 2)),
            dma((SLICES, 2)),
            dma((SLICES, 2)),
            dma((SLICES, 2)),
        ],
        compiler_params=pltpu.CompilerParams(
            collective_id=level, has_side_effects=True, vmem_limit_bytes=60 * 1024 * 1024
        ),
        name="adam_step",
    )(fix, *arrays)


def body(
    tokens, out_grad, step, up_param, down_param, up_first, down_first, up_second, down_second
):
    peers = lax.axis_size("peer")
    count = (step[0] + 1).astype(F32)
    first_fix = 1.0 - jnp.power(F32(0.9), count)
    second_fix = 1.0 - jnp.power(F32(0.999), count)
    fix = jnp.stack([0.01 / first_fix, 1.0 / second_fix])
    levels = peers.bit_length() - 1
    arrays = [
        a[0]
        for a in (
            tokens, out_grad, up_param, down_param, up_first, down_first, up_second, down_second
        )
    ]
    branches = [partial(fused, level, peers) for level in range(levels)]
    outs = lax.switch(step[0] % levels, branches, fix, *arrays)
    return tuple(o[None] for o in outs)


def solution(mesh):
    sharded = P("peer", "zero", None)
    return jax.shard_map(
        body,
        mesh=mesh,
        in_specs=(sharded, sharded, P()) + (sharded,) * 6,
        out_specs=(sharded,) * 6,
        check_vma=False,
    )
```

```python
from functools import partial

import jax
import jax.numpy as jnp
from jax import lax
from jax.experimental import pallas as pl
from jax.experimental.pallas import tpu as pltpu
from jax.sharding import PartitionSpec as P

MESH = pl.DeviceIdType.MESH
SLICES = 2
CHUNKS = 4
BF16 = jnp.bfloat16
F32 = jnp.float32


def dot(left, right, dims):
    return lax.dot_general(left, right, (dims, ((), ())), preferred_element_type=F32)


def kernel(
    peers,
    distance,
    fix,
    tokens,
    out_grad,
    up_param,
    down_param,
    up_first,
    down_first,
    up_second,
    down_second,
    up_p,
    dn_p,
    up_f,
    dn_f,
    up_s,
    dn_s,
    tok,
    grd,
    nrm,
    upw_send,
    upw,
    up_t,
    down_low,
    act,
    slope,
    acc_up,
    acc_down,
    ug_send,
    ug,
    dn_out,
    dn_in,
    up_out,
    up_in,
    dn_z,
    up_z,
    load_sem,
    far_send,
    far_recv,
    relay_send,
    relay_recv,
    near_send,
    near_recv,
    upw_ssem,
    upw_rsem,
    ug_ssem,
    ug_rsem,
    dn_ssem,
    dn_rsem,
    up_ssem,
    up_rsem,
    z_ssem,
    z_rsem,
):
    rows, width = tokens.shape
    hid = down_param.shape[0]
    part = up_param.shape[0]
    span = hid // SLICES
    piece = rows // CHUNKS
    block = 2 * piece
    own_blocks = rows // block
    blocks = tok.shape[0]
    near_blocks = 2 * own_blocks

    peer = lax.axis_index("peer")
    me = lax.axis_index("zero")
    mate = me + 1 - 2 * (me % 2)
    cross = (me + 2) % 4
    diagonal = 3 - me
    group = (cross, diagonal, mate)
    half = peers // 2
    twin = (peer + half) % peers
    if distance < half:
        upper = peer // half
        place = peer % half
        sends_on = place < distance
        gets_on = place + distance >= half
        onto = upper * half + (place + half - distance) % half
        source = upper * half + (place + distance) % half
    else:
        sends_on = gets_on = None
        onto = source = twin

    def local(src, dst, sem):
        return pltpu.make_async_copy(src, dst, sem)

    def remote(src, dst, ssem, rsem, **where):
        return pltpu.make_async_remote_copy(
            src_ref=src, dst_ref=dst, send_sem=ssem, recv_sem=rsem, device_id=where, device_id_type=MESH
        )

    loads = [
        local(up_param, up_p, load_sem.at[0]),
        local(down_param, dn_p, load_sem.at[1]),
        local(down_first, dn_f, load_sem.at[2]),
        local(down_second, dn_s, load_sem.at[3]),
        local(up_first, up_f, load_sem.at[4]),
        local(up_second, up_s, load_sem.at[5]),
    ]
    for b in range(own_blocks):
        at = pl.ds(b * block, block)
        loads.append(local(tokens.at[at], tok.at[b], load_sem.at[6 + 2 * b]))
        loads.append(local(out_grad.at[at], grd.at[b], load_sem.at[7 + 2 * b]))
    loads[0].start()

    barrier = pltpu.get_barrier_semaphore()
    for other in group:
        pl.semaphore_signal(barrier, inc=1, device_id={"zero": other}, device_id_type=MESH)
    others = (onto, source) if sends_on is None else (onto, source, twin)
    for other in others:
        pl.semaphore_signal(barrier, inc=1, device_id={"peer": other}, device_id_type=MESH)
    for copy in loads[1:]:
        copy.start()

    def far(kind, i):
        src, dst = ((tokens, tok), (out_grad, grd))[kind]
        at = pl.ds(pl.multiple_of(i * piece, piece), piece)
        return remote(
            src.at[at],
            dst.at[near_blocks + i, pl.ds(0, piece)],
            far_send.at[kind, i],
            far_recv.at[kind, i],
            zero=cross,
        )

    def relay(kind, i):
        dst = (tok, grd)[kind]
        return remote(
            dst.at[near_blocks + i, pl.ds(0, piece)],
            dst.at[near_blocks + i, pl.ds(piece, piece)],
            relay_send.at[kind, i],
            relay_recv.at[kind, i],
            zero=mate,
        )

    def near(kind, b):
        src, dst = ((tokens, tok), (out_grad, grd))[kind]
        return remote(
            src.at[pl.ds(b * block, block)],
            dst.at[own_blocks + b],
            near_send.at[kind, b],
            near_recv.at[kind, b],
            zero=mate,
        )

    def weights(s, o):
        return remote(
            upw_send.at[s, group[o]], upw.at[s, me], upw_ssem.at[s, o], upw_rsem.at[s, o], zero=group[o]
        )

    def weights_in(s, o):
        return remote(
            upw_send.at[s, group[o]], upw.at[s, group[o]], upw_ssem.at[s, o], upw_rsem.at[s, o], zero=group[o]
        )

    def grads(s, o):
        return remote(ug_send.at[s, group[o]], ug.at[s, me], ug_ssem.at[s, o], ug_rsem.at[s, o], zero=group[o])

    def grads_in(s, o):
        return remote(
            ug_send.at[s, group[o]], ug.at[s, group[o]], ug_ssem.at[s, o], ug_rsem.at[s, o], zero=group[o]
        )

    def cut(s, k):
        if k < 2:
            at = pl.ds(k * (span // 2), span // 2)
            return [ref.at[s, at] for ref in (dn_out, dn_in, dn_z)]
        at = pl.ds(2 * (k - 2), 2)
        return [ref.at[s, at] for ref in (up_out, up_in, up_z)]

    def away(s, k):
        out, into, _ = cut(s, k)
        sem = (dn_ssem, dn_rsem) if k < 2 else (up_ssem, up_rsem)
        return remote(out, into, sem[0].at[s, k % 2], sem[1].at[s, k % 2], peer=onto)

    def away_later(s, k):
        _, into, along = cut(s, k)
        sem = (dn_ssem, dn_rsem) if k < 2 else (up_ssem, up_rsem)
        return remote(along, into, sem[0].at[s, k % 2], sem[1].at[s, k % 2], peer=onto)

    def along_z(s, k):
        out, into, along = cut(s, k)
        return remote(out if s else into, along, z_ssem.at[s, k], z_rsem.at[s, k], peer=twin)

    def when(flag, run):
        if flag is not None:
            pl.when(flag)(run)

    def when_not(flag, run):
        if flag is None:
            run()
        else:
            pl.when(jnp.logical_not(flag))(run)

    pl.semaphore_wait(barrier, len(group) + len(others))
    far(0, 0).start()
    for kind in range(2):
        for b in range(own_blocks):
            near(kind, b).start()

    loads[0].wait()
    for s in range(SLICES):

        def lower(j, carry):
            at = pl.ds(pl.multiple_of(j * hid + s * span, span), span)
            upw_send[s, j] = up_p[:, at].astype(BF16)
            return carry

        lax.fori_loop(0, 4, lower, 0)
    for o in range(3):
        weights(0, o).start()
    far(1, 0).start()
    for i in range(1, CHUNKS):
        far(0, i).start()
        far(1, i).start()
    for s in range(1, SLICES):
        for o in range(3):
            weights(s, o).start()

    for s in range(SLICES):
        upw[s, me] = upw_send[s, me]
    loads[1].wait()

    def lower_down(r, carry):
        at = pl.ds(pl.multiple_of(r * (hid // 8), hid // 8), hid // 8)
        down_low[at] = dn_p[at].astype(BF16)
        return carry

    lax.fori_loop(0, 8, lower_down, 0)
    for copy in loads[6:]:
        copy.wait()

    def arrange(s):
        for o in range(3):
            weights_in(s, o).wait_recv()

        def turn(j, carry):
            up_t[:, pl.ds(pl.multiple_of(j * part, part), part)] = upw[s, j].astype(F32).T.astype(BF16)
            return carry

        lax.fori_loop(0, 4, turn, 0)

    def forward(b):
        pre = dot(up_t[...], nrm[b], ((1,), (1,)))
        cube = 0.044715 * pre * pre
        t = jnp.tanh(0.7978845608 * (pre + cube * pre))
        half = 0.5 * (1.0 + t)
        act[...] = (pre * half).astype(BF16)
        slope[...] = half + 0.5 * pre * (1.0 - t * t) * (0.7978845608 * (1.0 + 3.0 * cube))

    def gradients(s, b):
        act_grad = dot(down_low[pl.ds(s * span, span)], grd[b], ((1,), (1,)))
        pre_grad = (act_grad * slope[...]).astype(BF16)
        down = dot(act[...], grd[b], ((1,), (0,)))
        up = dot(pre_grad, nrm[b], ((1,), (0,)))
        acc_down[...] += down
        acc_up[...] += up

    def clear():
        acc_down[...] = jnp.zeros_like(acc_down)
        acc_up[...] = jnp.zeros_like(acc_up)

    def normalise(b):
        step = block // 4

        def some(r, carry):
            at = pl.ds(pl.multiple_of(r * step, step), step)
            wide = tok[b, at].astype(F32)
            center = jnp.mean(wide, axis=1, keepdims=True)
            wide = wide - center
            spread = jnp.mean(wide * wide, axis=1, keepdims=True)
            nrm[b, at] = (wide * lax.rsqrt(spread + 1e-05)).astype(BF16)
            return carry

        lax.fori_loop(0, 4, some, 0)

    def adam(param, first, second, grad):
        first_new = 0.9 * first + 0.1 * grad
        second_new = 0.999 * second + 0.001 * grad * grad
        step = (fix[0] * first_new) / (jnp.sqrt(second_new * fix[1]) + 1e-08)
        return param - step, first_new, second_new

    def down_update(s):
        tall = span // 4

        def some(r, carry):
            here = pl.ds(pl.multiple_of(r * tall, tall), tall)
            at = pl.ds(pl.multiple_of(s * span + r * tall, tall), tall)
            fresh = adam(dn_p[at], dn_f[at], dn_s[at], acc_down[here])
            dn_p[at], dn_f[at], dn_s[at] = fresh
            dn_out[s, here] = fresh[0].astype(BF16)
            return carry

        lax.fori_loop(0, 4, some, 0)

    def up_update(s):
        def some(j, carry):
            at = pl.ds(pl.multiple_of(j * hid + s * span, span), span)
            fresh = adam(up_p[:, at], up_f[:, at], up_s[:, at], ug[s, j].astype(F32))
            up_p[:, at], up_f[:, at], up_s[:, at] = fresh
            up_out[s, j] = fresh[0].astype(BF16)
            return carry

        lax.fori_loop(0, 4, some, 0)

    def share(s):
        def turn(j, carry):
            at = pl.ds(pl.multiple_of(j * part, part), part)
            ug_send[s, j] = acc_up[:, at].T.astype(BF16)
            return carry

        lax.fori_loop(0, 4, turn, 0)

    clear()
    arrange(0)

    def first_pass(b, carry):
        i = jnp.maximum(b - near_blocks, 0)

        @pl.when(jnp.logical_and(b >= own_blocks, b < near_blocks))
        def _():
            remote_near(0, b).wait_recv()

        @pl.when(b >= near_blocks)
        def _():
            far(0, i).wait_recv()
            relay(0, i).start()
            relay(0, i).wait_recv()

        normalise(b)
        forward(b)

        @pl.when(jnp.logical_and(b >= own_blocks, b < near_blocks))
        def _():
            remote_near(1, b).wait_recv()

        @pl.when(b >= near_blocks)
        def _():
            far(1, i).wait_recv()
            relay(1, i).start()
            relay(1, i).wait_recv()

        gradients(0, b)
        return carry

    def remote_near(kind, b):
        src, dst = ((tokens, tok), (out_grad, grd))[kind]
        n = jnp.clip(b - own_blocks, 0, own_blocks - 1)
        return remote(
            src.at[pl.ds(pl.multiple_of(n * block, block), block)],
            dst.at[own_blocks + n],
            near_send.at[kind, n],
            near_recv.at[kind, n],
            zero=mate,
        )

    lax.fori_loop(0, blocks, first_pass, 0)

    for copy in loads[2:6]:
        copy.wait()
    down_update(0)
    share(0)
    for k in range(2):
        away(0, k).start()
    ug[0, me] = ug_send[0, me]
    for o in range(3):
        grads(0, o).start()

    clear()
    arrange(1)

    def second_pass(b, carry):
        @pl.when(b == blocks // 2)
        def _():
            for o in range(3):
                grads_in(0, o).wait_recv()
            up_update(0)
            for k in range(2, 4):
                away(0, k).start()

        forward(b)
        gradients(1, b)
        return carry

    lax.fori_loop(0, blocks, second_pass, 0)
    share(1)
    down_update(1)
    for o in range(3):
        grads(1, o).start()
    ug[1, me] = ug_send[1, me]

    def start_down():
        for k in range(2):
            away(1, k).start()

    when_not(sends_on, start_down)

    for o in range(3):
        grads_in(1, o).wait_recv()
    up_update(1)

    def start_up():
        for k in range(2, 4):
            away(1, k).start()

    when_not(sends_on, start_up)
    for o in range(3):
        grads(1, o).wait_send()

    def pass_on():
        for k in range(4):
            away(0, k).wait_recv()
            along_z(0, k).start()

    when(gets_on, pass_on)

    def start_along():
        for k in range(4):
            along_z(1, k).start()

    when(sends_on, start_along)

    def go_on():
        for k in range(4):
            along_z(1, k).wait_recv()
            away_later(1, k).start()

    when(sends_on, go_on)

    def mean(s, k, down, up):
        if k < 2:
            tall = span // 2
            here = pl.ds(k * tall, tall)
            at = pl.ds(s * span + k * tall, tall)
            dn_p[at] = 0.5 * (dn_p[at] + down[s, here].astype(F32))
        else:
            for j in (2 * k - 4, 2 * k - 3):
                at = pl.ds(j * hid + s * span, span)
                up_p[:, at] = 0.5 * (up_p[:, at] + up[s, j].astype(F32))

    def means_near():
        for k in range(4):
            away(0, k).wait_recv()
            mean(0, k, dn_in, up_in)

    def means_along():
        for k in range(4):
            along_z(0, k).wait_recv()
            mean(0, k, dn_z, up_z)

    when_not(gets_on, means_near)
    when(gets_on, means_along)
    for k in range(4):
        away(1, k).wait_recv()
        mean(1, k, dn_in, up_in)

    for kind in range(2):
        for i in range(CHUNKS):
            far(kind, i).wait_send()
            relay(kind, i).wait_send()
        for b in range(own_blocks):
            near(kind, b).wait_send()
    for s in range(SLICES):
        for o in range(3):
            weights(s, o).wait_send()
    for o in range(3):
        grads(0, o).wait_send()
    for s in range(SLICES):
        for k in range(4):
            away(s, k).wait_send()

    def sent_along(s):
        for k in range(4):
            along_z(s, k).wait_send()

    when(gets_on, partial(sent_along, 0))
    when(sends_on, partial(sent_along, 1))


def flush_kernel(*refs):
    held, out, sem = refs[:6], refs[6:12], refs[12]
    copies = [pltpu.make_async_copy(held[i], out[i], sem.at[i]) for i in range(6)]
    for copy in copies:
        copy.start()
    for copy in copies:
        copy.wait()


def flush(*arrays):
    return pl.pallas_call(
        flush_kernel,
        out_shape=[jax.ShapeDtypeStruct(a.shape, a.dtype) for a in arrays],
        in_specs=[pl.BlockSpec(memory_space=pl.ANY)] * 6,
        out_specs=[pl.BlockSpec(memory_space=pl.ANY)] * 6,
        scratch_shapes=[pltpu.SemaphoreType.DMA((6,))],
        compiler_params=pltpu.CompilerParams(vmem_limit_bytes=4 * 1024 * 1024),
        name="flush",
    )(*arrays)


def fused(level, peers, fix, *arrays):
    tokens, out_grad, up_param, down_param = arrays[:4]
    rows, width = tokens.shape
    hid = down_param.shape[0]
    part, full = up_param.shape
    span = hid // SLICES
    piece = rows // CHUNKS
    block = 2 * piece
    blocks = 4 * rows // block
    own_blocks = rows // block
    dma = pltpu.SemaphoreType.DMA
    vmem = pltpu.VMEM
    shapes = [
        pltpu.VMEM(up_param.shape, F32),
        pltpu.VMEM(down_param.shape, F32),
    ] * 3
    return pl.pallas_call(
        partial(kernel, peers, 2**level),
        out_shape=shapes,
        in_specs=[pl.BlockSpec(memory_space=pltpu.SMEM)] + [pl.BlockSpec(memory_space=pl.ANY)] * 8,
        out_specs=[pl.BlockSpec(memory_space=pltpu.VMEM)] * 6,
        scratch_shapes=[
            vmem((blocks, block, width), BF16),
            vmem((blocks, block, width), BF16),
            vmem((blocks, block, width), BF16),
            vmem((SLICES, 4, part, span), BF16),
            vmem((SLICES, 4, part, span), BF16),
            vmem((span, width), BF16),
            vmem((hid, width), BF16),
            vmem((span, block), BF16),
            vmem((span, block), F32),
            vmem((span, width), F32),
            vmem((span, width), F32),
            vmem((SLICES, 4, part, span), BF16),
            vmem((SLICES, 4, part, span), BF16),
            vmem((SLICES, span, width), BF16),
            vmem((SLICES, span, width), BF16),
            vmem((SLICES, 4, part, span), BF16),
            vmem((SLICES, 4, part, span), BF16),
            vmem((SLICES, span, width), BF16),
            vmem((SLICES, 4, part, span), BF16),
            dma((6 + 2 * own_blocks,)),
            dma((2, CHUNKS)),
            dma((2, CHUNKS)),
            dma((2, CHUNKS)),
            dma((2, CHUNKS)),
            dma((2, own_blocks)),
            dma((2, own_blocks)),
            dma((SLICES, 3)),
            dma((SLICES, 3)),
            dma((SLICES, 3)),
            dma((SLICES, 3)),
            dma((SLICES, 2)),
            dma((SLICES, 2)),
            dma((SLICES, 2)),
            dma((SLICES, 2)),
            dma((SLICES, 4)),
            dma((SLICES, 4)),
        ],
        compiler_params=pltpu.CompilerParams(
            collective_id=level, has_side_effects=True, vmem_limit_bytes=46 * 1024 * 1024
        ),
        name="adam_step",
    )(fix, *arrays)


def step_at(level, peers, fix, *arrays):
    return flush(*fused(level, peers, fix, *arrays))


def body(
    tokens, out_grad, step, up_param, down_param, up_first, down_first, up_second, down_second
):
    peers = lax.axis_size("peer")
    count = (step[0] + 1).astype(F32)
    first_fix = 1.0 - jnp.power(F32(0.9), count)
    second_fix = 1.0 - jnp.power(F32(0.999), count)
    fix = jnp.stack([0.01 / first_fix, 1.0 / second_fix])
    levels = peers.bit_length() - 1
    arrays = [
        a[0]
        for a in (
            tokens, out_grad, up_param, down_param, up_first, down_first, up_second, down_second
        )
    ]
    branches = [partial(step_at, level, peers) for level in range(levels)]
    outs = lax.switch(step[0] % levels, branches, fix, *arrays)
    return tuple(o[None] for o in outs)


def solution(mesh):
    sharded = P("peer", "zero", None)
    return jax.shard_map(
        body,
        mesh=mesh,
        in_specs=(sharded, sharded, P()) + (sharded,) * 6,
        out_specs=(sharded,) * 6,
        check_vma=False,
    )
```

```python
from functools import partial

import jax
import jax.numpy as jnp
from jax import lax
from jax.experimental import pallas as pl
from jax.experimental.pallas import tpu as pltpu
from jax.sharding import PartitionSpec as P

MESH = pl.DeviceIdType.MESH
SLICES = 2
CHUNKS = 4
Z_FIRST = ((1, 1), (1, 2), (1, 3))
BF16 = jnp.bfloat16
F32 = jnp.float32


def dot(left, right, dims):
    return lax.dot_general(left, right, (dims, ((), ())), preferred_element_type=F32)


def kernel(
    peers,
    distance,
    fix,
    tokens,
    out_grad,
    up_param,
    down_param,
    up_first,
    down_first,
    up_second,
    down_second,
    up_p,
    dn_p,
    up_f,
    dn_f,
    up_s,
    dn_s,
    tok,
    grd,
    nrm,
    upw_send,
    upw,
    up_t,
    down_low,
    act,
    slope,
    acc_up,
    acc_down,
    ug_send,
    ug,
    dn_out,
    dn_in,
    up_out,
    up_in,
    dn_z,
    up_z,
    load_sem,
    far_send,
    far_recv,
    relay_send,
    relay_recv,
    near_send,
    near_recv,
    upw_ssem,
    upw_rsem,
    ug_ssem,
    ug_rsem,
    dn_ssem,
    dn_rsem,
    up_ssem,
    up_rsem,
    z_ssem,
    z_rsem,
):
    rows, width = tokens.shape
    hid = down_param.shape[0]
    part = up_param.shape[0]
    span = hid // SLICES
    piece = rows // CHUNKS
    block = 2 * piece
    own_blocks = rows // block
    blocks = tok.shape[0]
    near_blocks = 2 * own_blocks

    peer = lax.axis_index("peer")
    me = lax.axis_index("zero")
    mate = me + 1 - 2 * (me % 2)
    cross = (me + 2) % 4
    diagonal = 3 - me
    group = (cross, diagonal, mate)
    half = peers // 2
    twin = (peer + half) % peers
    if distance < half:
        upper = peer // half
        place = peer % half
        sends_on = place < distance
        gets_on = place + distance >= half
        onto = upper * half + (place + half - distance) % half
        source = upper * half + (place + distance) % half
    else:
        sends_on = gets_on = None
        onto = source = twin

    def local(src, dst, sem):
        return pltpu.make_async_copy(src, dst, sem)

    def remote(src, dst, ssem, rsem, **where):
        return pltpu.make_async_remote_copy(
            src_ref=src, dst_ref=dst, send_sem=ssem, recv_sem=rsem, device_id=where, device_id_type=MESH
        )

    loads = [
        local(up_param, up_p, load_sem.at[0]),
        local(down_param, dn_p, load_sem.at[1]),
        local(down_first, dn_f, load_sem.at[2]),
        local(down_second, dn_s, load_sem.at[3]),
        local(up_first, up_f, load_sem.at[4]),
        local(up_second, up_s, load_sem.at[5]),
    ]
    for b in range(own_blocks):
        at = pl.ds(b * block, block)
        loads.append(local(tokens.at[at], tok.at[b], load_sem.at[6 + 2 * b]))
        loads.append(local(out_grad.at[at], grd.at[b], load_sem.at[7 + 2 * b]))
    loads[0].start()

    barrier = pltpu.get_barrier_semaphore()
    for other in group:
        pl.semaphore_signal(barrier, inc=1, device_id={"zero": other}, device_id_type=MESH)
    others = (onto, source) if sends_on is None else (onto, source, twin)
    for other in others:
        pl.semaphore_signal(barrier, inc=1, device_id={"peer": other}, device_id_type=MESH)
    for copy in loads[1:]:
        copy.start()

    def far(kind, i):
        src, dst = ((tokens, tok), (out_grad, grd))[kind]
        at = pl.ds(pl.multiple_of(i * piece, piece), piece)
        return remote(
            src.at[at],
            dst.at[near_blocks + i, pl.ds(0, piece)],
            far_send.at[kind, i],
            far_recv.at[kind, i],
            zero=cross,
        )

    def relay(kind, i):
        dst = (tok, grd)[kind]
        return remote(
            dst.at[near_blocks + i, pl.ds(0, piece)],
            dst.at[near_blocks + i, pl.ds(piece, piece)],
            relay_send.at[kind, i],
            relay_recv.at[kind, i],
            zero=mate,
        )

    def near(kind, b):
        src, dst = ((tokens, tok), (out_grad, grd))[kind]
        return remote(
            src.at[pl.ds(b * block, block)],
            dst.at[own_blocks + b],
            near_send.at[kind, b],
            near_recv.at[kind, b],
            zero=mate,
        )

    def weights(s, o):
        return remote(
            upw_send.at[s, group[o]], upw.at[s, me], upw_ssem.at[s, o], upw_rsem.at[s, o], zero=group[o]
        )

    def weights_in(s, o):
        return remote(
            upw_send.at[s, group[o]], upw.at[s, group[o]], upw_ssem.at[s, o], upw_rsem.at[s, o], zero=group[o]
        )

    def grads(s, o):
        return remote(ug_send.at[s, group[o]], ug.at[s, me], ug_ssem.at[s, o], ug_rsem.at[s, o], zero=group[o])

    def grads_in(s, o):
        return remote(
            ug_send.at[s, group[o]], ug.at[s, group[o]], ug_ssem.at[s, o], ug_rsem.at[s, o], zero=group[o]
        )

    def cut(s, k):
        if k < 2:
            at = pl.ds(k * (span // 2), span // 2)
            return [ref.at[s, at] for ref in (dn_out, dn_in, dn_z)]
        at = pl.ds(2 * (k - 2), 2)
        return [ref.at[s, at] for ref in (up_out, up_in, up_z)]

    def away(s, k):
        out, into, _ = cut(s, k)
        sem = (dn_ssem, dn_rsem) if k < 2 else (up_ssem, up_rsem)
        return remote(out, into, sem[0].at[s, k % 2], sem[1].at[s, k % 2], peer=onto)

    def away_later(s, k):
        _, into, along = cut(s, k)
        sem = (dn_ssem, dn_rsem) if k < 2 else (up_ssem, up_rsem)
        return remote(along, into, sem[0].at[s, k % 2], sem[1].at[s, k % 2], peer=onto)

    def along_z(s, k):
        out, into, along = cut(s, k)
        return remote(out if (s, k) in Z_FIRST else into, along, z_ssem.at[s, k], z_rsem.at[s, k], peer=twin)

    def when(flag, run):
        if flag is not None:
            pl.when(flag)(run)

    def when_not(flag, run):
        if flag is None:
            run()
        else:
            pl.when(jnp.logical_not(flag))(run)

    pl.semaphore_wait(barrier, len(group) + len(others))
    far(0, 0).start()
    for kind in range(2):
        for b in range(own_blocks):
            near(kind, b).start()

    loads[0].wait()
    for s in range(SLICES):

        def lower(j, carry):
            at = pl.ds(pl.multiple_of(j * hid + s * span, span), span)
            upw_send[s, j] = up_p[:, at].astype(BF16)
            return carry

        lax.fori_loop(0, 4, lower, 0)
    for o in range(3):
        weights(0, o).start()
    far(1, 0).start()
    for i in range(1, CHUNKS):
        far(0, i).start()
        far(1, i).start()
    for s in range(1, SLICES):
        for o in range(3):
            weights(s, o).start()

    for s in range(SLICES):
        upw[s, me] = upw_send[s, me]
    loads[1].wait()

    def lower_down(r, carry):
        at = pl.ds(pl.multiple_of(r * (hid // 8), hid // 8), hid // 8)
        down_low[at] = dn_p[at].astype(BF16)
        return carry

    lax.fori_loop(0, 8, lower_down, 0)
    for copy in loads[6:]:
        copy.wait()

    def arrange(s):
        for o in range(3):
            weights_in(s, o).wait_recv()

        def turn(j, carry):
            up_t[:, pl.ds(pl.multiple_of(j * part, part), part)] = upw[s, j].astype(F32).T.astype(BF16)
            return carry

        lax.fori_loop(0, 4, turn, 0)

    def forward(b):
        pre = dot(up_t[...], nrm[b], ((1,), (1,)))
        cube = 0.044715 * pre * pre
        t = jnp.tanh(0.7978845608 * (pre + cube * pre))
        half = 0.5 * (1.0 + t)
        act[...] = (pre * half).astype(BF16)
        slope[...] = half + 0.5 * pre * (1.0 - t * t) * (0.7978845608 * (1.0 + 3.0 * cube))

    def gradients(s, b):
        act_grad = dot(down_low[pl.ds(s * span, span)], grd[b], ((1,), (1,)))
        pre_grad = (act_grad * slope[...]).astype(BF16)
        down = dot(act[...], grd[b], ((1,), (0,)))
        up = dot(pre_grad, nrm[b], ((1,), (0,)))
        acc_down[...] += down
        acc_up[...] += up

    def clear():
        acc_down[...] = jnp.zeros_like(acc_down)
        acc_up[...] = jnp.zeros_like(acc_up)

    def normalise(b):
        step = block // 4

        def some(r, carry):
            at = pl.ds(pl.multiple_of(r * step, step), step)
            wide = tok[b, at].astype(F32)
            center = jnp.mean(wide, axis=1, keepdims=True)
            wide = wide - center
            spread = jnp.mean(wide * wide, axis=1, keepdims=True)
            nrm[b, at] = (wide * lax.rsqrt(spread + 1e-05)).astype(BF16)
            return carry

        lax.fori_loop(0, 4, some, 0)

    def adam(param, first, second, grad):
        first_new = 0.9 * first + 0.1 * grad
        second_new = 0.999 * second + 0.001 * grad * grad
        step = (fix[0] * first_new) / (jnp.sqrt(second_new * fix[1]) + 1e-08)
        return param - step, first_new, second_new

    def down_update(s, k):
        tall = span // 4

        def some(r, carry):
            here = pl.ds(pl.multiple_of(r * tall, tall), tall)
            at = pl.ds(pl.multiple_of(s * span + r * tall, tall), tall)
            fresh = adam(dn_p[at], dn_f[at], dn_s[at], acc_down[here])
            dn_p[at], dn_f[at], dn_s[at] = fresh
            dn_out[s, here] = fresh[0].astype(BF16)
            return carry

        lax.fori_loop(2 * k, 2 * k + 2, some, 0)

    def up_update(s):
        def some(j, carry):
            at = pl.ds(pl.multiple_of(j * hid + s * span, span), span)
            fresh = adam(up_p[:, at], up_f[:, at], up_s[:, at], ug[s, j].astype(F32))
            up_p[:, at], up_f[:, at], up_s[:, at] = fresh
            up_out[s, j] = fresh[0].astype(BF16)
            return carry

        lax.fori_loop(0, 4, some, 0)

    def share(s):
        def turn(j, carry):
            at = pl.ds(pl.multiple_of(j * part, part), part)
            ug_send[s, j] = acc_up[:, at].T.astype(BF16)
            return carry

        lax.fori_loop(0, 4, turn, 0)

    clear()
    arrange(0)

    def first_pass(b, carry):
        i = jnp.maximum(b - near_blocks, 0)

        @pl.when(jnp.logical_and(b >= own_blocks, b < near_blocks))
        def _():
            remote_near(0, b).wait_recv()

        @pl.when(b >= near_blocks)
        def _():
            far(0, i).wait_recv()
            relay(0, i).start()
            relay(0, i).wait_recv()

        normalise(b)
        forward(b)

        @pl.when(jnp.logical_and(b >= own_blocks, b < near_blocks))
        def _():
            remote_near(1, b).wait_recv()

        @pl.when(b >= near_blocks)
        def _():
            far(1, i).wait_recv()
            relay(1, i).start()
            relay(1, i).wait_recv()

        gradients(0, b)
        return carry

    def remote_near(kind, b):
        src, dst = ((tokens, tok), (out_grad, grd))[kind]
        n = jnp.clip(b - own_blocks, 0, own_blocks - 1)
        return remote(
            src.at[pl.ds(pl.multiple_of(n * block, block), block)],
            dst.at[own_blocks + n],
            near_send.at[kind, n],
            near_recv.at[kind, n],
            zero=mate,
        )

    lax.fori_loop(0, blocks, first_pass, 0)

    for copy in loads[2:6]:
        copy.wait()
    down_update(0, 0)
    down_update(0, 1)
    away(0, 0).start()
    share(0)
    away(0, 1).start()
    ug[0, me] = ug_send[0, me]
    for o in range(3):
        grads(0, o).start()

    def pass_on(*pieces):
        def run():
            for s, k in pieces:
                away(s, k).wait_recv()
                along_z(s, k).start()

        when(gets_on, run)

    clear()
    arrange(1)

    def second_pass(b, carry):
        @pl.when(b == blocks // 2)
        def _():
            for o in range(3):
                grads_in(0, o).wait_recv()
            up_update(0)
            for k in range(2, 4):
                away(0, k).start()

        @pl.when(b == blocks - 2)
        def _():
            pass_on((0, 0), (0, 1))

        forward(b)
        gradients(1, b)
        return carry

    lax.fori_loop(0, blocks, second_pass, 0)
    share(1)
    down_update(1, 0)
    down_update(1, 1)
    ug[1, me] = ug_send[1, me]
    for o in range(3):
        grads(1, o).start()
    away(1, 0).start()

    def start_down():
        away(1, 1).start()

    when_not(sends_on, start_down)
    pass_on((0, 2))
    for o in range(3):
        grads_in(1, o).wait_recv()
    up_update(1)

    def start_up():
        for k in range(2, 4):
            away(1, k).start()

    def start_along():
        for s, k in Z_FIRST:
            along_z(s, k).start()

    when_not(sends_on, start_up)
    when(sends_on, start_along)
    pass_on((0, 3), (1, 0))

    def go_on():
        for s, k in Z_FIRST:
            along_z(s, k).wait_recv()
            away_later(s, k).start()

    when(sends_on, go_on)

    def mean(s, k, down, up):
        if k < 2:
            tall = span // 2
            here = pl.ds(k * tall, tall)
            at = pl.ds(s * span + k * tall, tall)
            dn_p[at] = 0.5 * (dn_p[at] + down[s, here].astype(F32))
        else:
            for j in (2 * k - 4, 2 * k - 3):
                at = pl.ds(j * hid + s * span, span)
                up_p[:, at] = 0.5 * (up_p[:, at] + up[s, j].astype(F32))

    pieces = [(s, k) for s in range(SLICES) for k in range(4)]
    x_first = [piece for piece in pieces if piece not in Z_FIRST]

    def means_near():
        for s, k in x_first:
            away(s, k).wait_recv()
            mean(s, k, dn_in, up_in)

    def means_along():
        for s, k in x_first:
            along_z(s, k).wait_recv()
            mean(s, k, dn_z, up_z)

    when_not(gets_on, means_near)
    when(gets_on, means_along)
    for s, k in Z_FIRST:
        away(s, k).wait_recv()
        mean(s, k, dn_in, up_in)

    for kind in range(2):
        for i in range(CHUNKS):
            far(kind, i).wait_send()
            relay(kind, i).wait_send()
        for b in range(own_blocks):
            near(kind, b).wait_send()
    for s in range(SLICES):
        for o in range(3):
            weights(s, o).wait_send()
            grads(s, o).wait_send()
    for s, k in pieces:
        away(s, k).wait_send()

    def sent_along(some):
        for s, k in some:
            along_z(s, k).wait_send()

    when(gets_on, partial(sent_along, x_first))
    when(sends_on, partial(sent_along, Z_FIRST))


def flush_kernel(*refs):
    held, out, sem = refs[:6], refs[6:12], refs[12]
    copies = [pltpu.make_async_copy(held[i], out[i], sem.at[i]) for i in range(6)]
    for copy in copies:
        copy.start()
    for copy in copies:
        copy.wait()


def flush(*arrays):
    return pl.pallas_call(
        flush_kernel,
        out_shape=[jax.ShapeDtypeStruct(a.shape, a.dtype) for a in arrays],
        in_specs=[pl.BlockSpec(memory_space=pl.ANY)] * 6,
        out_specs=[pl.BlockSpec(memory_space=pl.ANY)] * 6,
        scratch_shapes=[pltpu.SemaphoreType.DMA((6,))],
        compiler_params=pltpu.CompilerParams(vmem_limit_bytes=4 * 1024 * 1024),
        name="flush",
    )(*arrays)


def fused(level, peers, fix, *arrays):
    tokens, out_grad, up_param, down_param = arrays[:4]
    rows, width = tokens.shape
    hid = down_param.shape[0]
    part, full = up_param.shape
    span = hid // SLICES
    piece = rows // CHUNKS
    block = 2 * piece
    blocks = 4 * rows // block
    own_blocks = rows // block
    dma = pltpu.SemaphoreType.DMA
    vmem = pltpu.VMEM
    shapes = [
        pltpu.VMEM(up_param.shape, F32),
        pltpu.VMEM(down_param.shape, F32),
    ] * 3
    return pl.pallas_call(
        partial(kernel, peers, 2**level),
        out_shape=shapes,
        in_specs=[pl.BlockSpec(memory_space=pltpu.SMEM)] + [pl.BlockSpec(memory_space=pl.ANY)] * 8,
        out_specs=[pl.BlockSpec(memory_space=pltpu.VMEM)] * 6,
        scratch_shapes=[
            vmem((blocks, block, width), BF16),
            vmem((blocks, block, width), BF16),
            vmem((blocks, block, width), BF16),
            vmem((SLICES, 4, part, span), BF16),
            vmem((SLICES, 4, part, span), BF16),
            vmem((span, width), BF16),
            vmem((hid, width), BF16),
            vmem((span, block), BF16),
            vmem((span, block), F32),
            vmem((span, width), F32),
            vmem((span, width), F32),
            vmem((SLICES, 4, part, span), BF16),
            vmem((SLICES, 4, part, span), BF16),
            vmem((SLICES, span, width), BF16),
            vmem((SLICES, span, width), BF16),
            vmem((SLICES, 4, part, span), BF16),
            vmem((SLICES, 4, part, span), BF16),
            vmem((SLICES, span, width), BF16),
            vmem((SLICES, 4, part, span), BF16),
            dma((6 + 2 * own_blocks,)),
            dma((2, CHUNKS)),
            dma((2, CHUNKS)),
            dma((2, CHUNKS)),
            dma((2, CHUNKS)),
            dma((2, own_blocks)),
            dma((2, own_blocks)),
            dma((SLICES, 3)),
            dma((SLICES, 3)),
            dma((SLICES, 3)),
            dma((SLICES, 3)),
            dma((SLICES, 2)),
            dma((SLICES, 2)),
            dma((SLICES, 2)),
            dma((SLICES, 2)),
            dma((SLICES, 4)),
            dma((SLICES, 4)),
        ],
        compiler_params=pltpu.CompilerParams(
            collective_id=level, has_side_effects=True, vmem_limit_bytes=46 * 1024 * 1024
        ),
        name="adam_step",
    )(fix, *arrays)


def step_at(level, peers, fix, *arrays):
    return flush(*fused(level, peers, fix, *arrays))


def body(
    tokens, out_grad, step, up_param, down_param, up_first, down_first, up_second, down_second
):
    peers = lax.axis_size("peer")
    count = (step[0] + 1).astype(F32)
    first_fix = 1.0 - jnp.power(F32(0.9), count)
    second_fix = 1.0 - jnp.power(F32(0.999), count)
    fix = jnp.stack([0.01 / first_fix, 1.0 / second_fix])
    levels = peers.bit_length() - 1
    arrays = [
        a[0]
        for a in (
            tokens, out_grad, up_param, down_param, up_first, down_first, up_second, down_second
        )
    ]
    branches = [partial(step_at, level, peers) for level in range(levels)]
    outs = lax.switch(step[0] % levels, branches, fix, *arrays)
    return tuple(o[None] for o in outs)


def solution(mesh):
    sharded = P("peer", "zero", None)
    return jax.shard_map(
        body,
        mesh=mesh,
        in_specs=(sharded, sharded, P()) + (sharded,) * 6,
        out_specs=(sharded,) * 6,
        check_vma=False,
    )
```

```python
from functools import partial

import jax
import jax.numpy as jnp
from jax import lax
from jax.experimental import pallas as pl
from jax.experimental.pallas import tpu as pltpu
from jax.sharding import PartitionSpec as P

MESH = pl.DeviceIdType.MESH
SLICES = 4
CHUNKS = 4
Z_FIRST = ((1, 2), (1, 3), (3, 0), (3, 1), (3, 2), (3, 3))
ON_LOOP = {1: ((0, 0), (0, 1))}
ON_AFTER = {2: ((0, 2), (0, 3)), 3: ((1, 0), (1, 1), (2, 0), (2, 1))}
ON_LAST = ((2, 2), (2, 3))
GO_LOOP = {3: ((1, 2), (1, 3))}
GO_LAST = ((3, 0), (3, 1), (3, 2), (3, 3))
BF16 = jnp.bfloat16
F32 = jnp.float32


def dot(left, right, dims):
    return lax.dot_general(left, right, (dims, ((), ())), preferred_element_type=F32)


def kernel(
    peers,
    distance,
    fix,
    tokens,
    out_grad,
    up_param,
    down_param,
    up_first,
    down_first,
    up_second,
    down_second,
    up_p,
    dn_p,
    up_f,
    dn_f,
    up_s,
    dn_s,
    tok,
    grd,
    nrm,
    upw_send,
    upw,
    up_t,
    down_low,
    act,
    slope,
    acc_up,
    acc_down,
    ug_send,
    ug,
    dn_out,
    dn_in,
    up_out,
    up_in,
    dn_z,
    up_z,
    load_sem,
    far_send,
    far_recv,
    relay_send,
    relay_recv,
    near_send,
    near_recv,
    upw_ssem,
    upw_rsem,
    ug_ssem,
    ug_rsem,
    away_ssem,
    away_rsem,
    z_ssem,
    z_rsem,
):
    rows, width = tokens.shape
    hid = down_param.shape[0]
    part = up_param.shape[0]
    span = hid // SLICES
    piece = rows // CHUNKS
    block = 2 * piece
    own_blocks = rows // block
    blocks = tok.shape[0]
    near_blocks = 2 * own_blocks

    peer = lax.axis_index("peer")
    me = lax.axis_index("zero")
    mate = me + 1 - 2 * (me % 2)
    cross = (me + 2) % 4
    diagonal = 3 - me
    group = (cross, diagonal, mate)
    half = peers // 2
    twin = (peer + half) % peers
    if distance < half:
        upper = peer // half
        place = peer % half
        sends_on = place < distance
        gets_on = place + distance >= half
        onto = upper * half + (place + half - distance) % half
        source = upper * half + (place + distance) % half
    else:
        sends_on = gets_on = None
        onto = source = twin

    def local(src, dst, sem):
        return pltpu.make_async_copy(src, dst, sem)

    def remote(src, dst, ssem, rsem, **where):
        return pltpu.make_async_remote_copy(
            src_ref=src, dst_ref=dst, send_sem=ssem, recv_sem=rsem, device_id=where, device_id_type=MESH
        )

    loads = [
        local(up_param, up_p, load_sem.at[0]),
        local(down_param, dn_p, load_sem.at[1]),
        local(down_first, dn_f, load_sem.at[2]),
        local(down_second, dn_s, load_sem.at[3]),
        local(up_first, up_f, load_sem.at[4]),
        local(up_second, up_s, load_sem.at[5]),
    ]
    for b in range(own_blocks):
        at = pl.ds(b * block, block)
        loads.append(local(tokens.at[at], tok.at[b], load_sem.at[6 + 2 * b]))
        loads.append(local(out_grad.at[at], grd.at[b], load_sem.at[7 + 2 * b]))
    loads[0].start()

    barrier = pltpu.get_barrier_semaphore()
    for other in group:
        pl.semaphore_signal(barrier, inc=1, device_id={"zero": other}, device_id_type=MESH)
    others = (onto, source) if sends_on is None else (onto, source, twin)
    for other in others:
        pl.semaphore_signal(barrier, inc=1, device_id={"peer": other}, device_id_type=MESH)
    for copy in loads[1:]:
        copy.start()

    def far(kind, i):
        src, dst = ((tokens, tok), (out_grad, grd))[kind]
        at = pl.ds(pl.multiple_of(i * piece, piece), piece)
        return remote(
            src.at[at],
            dst.at[near_blocks + i, pl.ds(0, piece)],
            far_send.at[kind, i],
            far_recv.at[kind, i],
            zero=cross,
        )

    def relay(kind, i):
        dst = (tok, grd)[kind]
        return remote(
            dst.at[near_blocks + i, pl.ds(0, piece)],
            dst.at[near_blocks + i, pl.ds(piece, piece)],
            relay_send.at[kind, i],
            relay_recv.at[kind, i],
            zero=mate,
        )

    def near(kind, b):
        src, dst = ((tokens, tok), (out_grad, grd))[kind]
        return remote(
            src.at[pl.ds(b * block, block)],
            dst.at[own_blocks + b],
            near_send.at[kind, b],
            near_recv.at[kind, b],
            zero=mate,
        )

    def weights(s, o):
        return remote(
            upw_send.at[s, group[o]], upw.at[s, me], upw_ssem.at[s, o], upw_rsem.at[s, o], zero=group[o]
        )

    def weights_in(s, o):
        return remote(
            upw_send.at[s, group[o]], upw.at[s, group[o]], upw_ssem.at[s, o], upw_rsem.at[s, o], zero=group[o]
        )

    def grads(s, o):
        return remote(ug_send.at[s, group[o]], ug.at[s, me], ug_ssem.at[s, o], ug_rsem.at[s, o], zero=group[o])

    def grads_in(s, o):
        return remote(
            ug_send.at[s, group[o]], ug.at[s, group[o]], ug_ssem.at[s, o], ug_rsem.at[s, o], zero=group[o]
        )

    def cut(s, k):
        if k < 2:
            at = pl.ds(k * (span // 2), span // 2)
            return [ref.at[s, at] for ref in (dn_out, dn_in, dn_z)]
        at = pl.ds(2 * (k - 2), 2)
        return [ref.at[s, at] for ref in (up_out, up_in, up_z)]

    def away(s, k):
        out, into, _ = cut(s, k)
        return remote(out, into, away_ssem.at[s, k], away_rsem.at[s, k], peer=onto)

    def away_later(s, k):
        _, into, along = cut(s, k)
        return remote(along, into, away_ssem.at[s, k], away_rsem.at[s, k], peer=onto)

    def along_z(s, k):
        out, into, along = cut(s, k)
        return remote(out if (s, k) in Z_FIRST else into, along, z_ssem.at[s, k], z_rsem.at[s, k], peer=twin)

    def when(flag, run):
        if flag is not None:
            pl.when(flag)(run)

    def when_not(flag, run):
        if flag is None:
            run()
        else:
            pl.when(jnp.logical_not(flag))(run)

    pl.semaphore_wait(barrier, len(group) + len(others))
    far(0, 0).start()
    for kind in range(2):
        for b in range(own_blocks):
            near(kind, b).start()

    loads[0].wait()
    for s in range(SLICES):

        def lower(j, carry):
            at = pl.ds(pl.multiple_of(j * hid + s * span, span), span)
            upw_send[s, j] = up_p[:, at].astype(BF16)
            return carry

        lax.fori_loop(0, 4, lower, 0)
    for o in range(3):
        weights(0, o).start()
    far(1, 0).start()
    for i in range(1, CHUNKS):
        far(0, i).start()
        far(1, i).start()
    for o in range(3):
        weights(1, o).start()

    for s in range(SLICES):
        upw[s, me] = upw_send[s, me]
    loads[1].wait()

    def lower_down(r, carry):
        at = pl.ds(pl.multiple_of(r * (hid // 8), hid // 8), hid // 8)
        down_low[at] = dn_p[at].astype(BF16)
        return carry

    lax.fori_loop(0, 8, lower_down, 0)
    for copy in loads[6:]:
        copy.wait()

    def arrange(s):
        for o in range(3):
            weights_in(s, o).wait_recv()

        def turn(j, carry):
            up_t[:, pl.ds(pl.multiple_of(j * part, part), part)] = upw[s, j].astype(F32).T.astype(BF16)
            return carry

        lax.fori_loop(0, 4, turn, 0)

    def forward(b):
        pre = dot(up_t[...], nrm[b], ((1,), (1,)))
        cube = 0.044715 * pre * pre
        t = jnp.tanh(0.7978845608 * (pre + cube * pre))
        half = 0.5 * (1.0 + t)
        act[...] = (pre * half).astype(BF16)
        slope[...] = half + 0.5 * pre * (1.0 - t * t) * (0.7978845608 * (1.0 + 3.0 * cube))

    def gradients(s, b):
        act_grad = dot(down_low[pl.ds(s * span, span)], grd[b], ((1,), (1,)))
        pre_grad = (act_grad * slope[...]).astype(BF16)
        down = dot(act[...], grd[b], ((1,), (0,)))
        up = dot(pre_grad, nrm[b], ((1,), (0,)))
        acc_down[...] += down
        acc_up[...] += up

    def clear():
        acc_down[...] = jnp.zeros_like(acc_down)
        acc_up[...] = jnp.zeros_like(acc_up)

    def normalise(b):
        step = block // 4

        def some(r, carry):
            at = pl.ds(pl.multiple_of(r * step, step), step)
            wide = tok[b, at].astype(F32)
            center = jnp.mean(wide, axis=1, keepdims=True)
            wide = wide - center
            spread = jnp.mean(wide * wide, axis=1, keepdims=True)
            nrm[b, at] = (wide * lax.rsqrt(spread + 1e-05)).astype(BF16)
            return carry

        lax.fori_loop(0, 4, some, 0)

    def adam(param, first, second, grad):
        first_new = 0.9 * first + 0.1 * grad
        second_new = 0.999 * second + 0.001 * grad * grad
        step = (fix[0] * first_new) / (jnp.sqrt(second_new * fix[1]) + 1e-08)
        return param - step, first_new, second_new

    def down_update(s):
        tall = span // 2

        def some(r, carry):
            here = pl.ds(pl.multiple_of(r * tall, tall), tall)
            at = pl.ds(pl.multiple_of(s * span + r * tall, tall), tall)
            fresh = adam(dn_p[at], dn_f[at], dn_s[at], acc_down[here])
            dn_p[at], dn_f[at], dn_s[at] = fresh
            dn_out[s, here] = fresh[0].astype(BF16)
            return carry

        lax.fori_loop(0, 2, some, 0)

    def up_update(s):
        def some(j, carry):
            at = pl.ds(pl.multiple_of(j * hid + s * span, span), span)
            fresh = adam(up_p[:, at], up_f[:, at], up_s[:, at], ug[s, j].astype(F32))
            up_p[:, at], up_f[:, at], up_s[:, at] = fresh
            up_out[s, j] = fresh[0].astype(BF16)
            return carry

        lax.fori_loop(0, 4, some, 0)

    def share(s):
        def turn(j, carry):
            at = pl.ds(pl.multiple_of(j * part, part), part)
            ug_send[s, j] = acc_up[:, at].T.astype(BF16)
            return carry

        lax.fori_loop(0, 4, turn, 0)

    clear()
    arrange(0)

    def first_pass(b, carry):
        i = jnp.maximum(b - near_blocks, 0)

        @pl.when(jnp.logical_and(b >= own_blocks, b < near_blocks))
        def _():
            remote_near(0, b).wait_recv()

        @pl.when(b >= near_blocks)
        def _():
            far(0, i).wait_recv()
            relay(0, i).start()
            relay(0, i).wait_recv()

        normalise(b)
        forward(b)

        @pl.when(jnp.logical_and(b >= own_blocks, b < near_blocks))
        def _():
            remote_near(1, b).wait_recv()

        @pl.when(b >= near_blocks)
        def _():
            far(1, i).wait_recv()
            relay(1, i).start()
            relay(1, i).wait_recv()

        gradients(0, b)
        return carry

    def remote_near(kind, b):
        src, dst = ((tokens, tok), (out_grad, grd))[kind]
        n = jnp.clip(b - own_blocks, 0, own_blocks - 1)
        return remote(
            src.at[pl.ds(pl.multiple_of(n * block, block), block)],
            dst.at[own_blocks + n],
            near_send.at[kind, n],
            near_recv.at[kind, n],
            zero=mate,
        )

    lax.fori_loop(0, blocks, first_pass, 0)

    for copy in loads[2:6]:
        copy.wait()

    def depart(s, k):
        if (s, k) in Z_FIRST:
            when_not(sends_on, lambda: away(s, k).start())
            if sends_on is not None:
                when(sends_on, lambda: along_z(s, k).start())
        else:
            away(s, k).start()

    def pass_on(pieces):
        def run():
            for s, k in pieces:
                away(s, k).wait_recv()
                along_z(s, k).start()

        if pieces:
            when(gets_on, run)

    def go_on(pieces):
        def run():
            for s, k in pieces:
                along_z(s, k).wait_recv()
                away_later(s, k).start()

        if pieces:
            when(sends_on, run)

    def exchange(s):
        ug[s, me] = ug_send[s, me]
        for o in range(3):
            grads(s, o).start()
        if s + 2 < SLICES:
            for o in range(3):
                weights(s + 2, o).start()

    def finish(s):
        share(s)
        exchange(s)
        down_update(s)
        depart(s, 0)
        depart(s, 1)

    def finish_up(s):
        for o in range(3):
            grads_in(s, o).wait_recv()
        up_update(s)
        depart(s, 2)
        depart(s, 3)

    finish(0)

    for s in range(1, SLICES):
        clear()
        arrange(s)

        def pass_over(b, carry, s=s):
            @pl.when(b == (blocks - 3 if s == 1 else blocks - 2))
            def _():
                finish_up(s - 1)

            if s in ON_LOOP or s in GO_LOOP:

                @pl.when(b == blocks - 1)
                def _():
                    pass_on(ON_LOOP.get(s))
                    go_on(GO_LOOP.get(s))

            forward(b)
            gradients(s, b)
            return carry

        lax.fori_loop(0, blocks, pass_over, 0)
        finish(s)
        pass_on(ON_AFTER.get(s))
    finish_up(SLICES - 1)
    pass_on(ON_LAST)

    go_on(GO_LAST)

    def mean(s, k, down, up):
        if k < 2:
            tall = span // 2
            at = pl.ds(s * span + k * tall, tall)
            dn_p[at] = 0.5 * (dn_p[at] + down[s, pl.ds(k * tall, tall)].astype(F32))
        else:
            for j in (2 * k - 4, 2 * k - 3):
                at = pl.ds(j * hid + s * span, span)
                up_p[:, at] = 0.5 * (up_p[:, at] + up[s, j].astype(F32))

    pieces = [(s, k) for s in range(SLICES) for k in range(4)]
    x_first = [piece for piece in pieces if piece not in Z_FIRST]

    def means_near():
        for s, k in x_first:
            away(s, k).wait_recv()
            mean(s, k, dn_in, up_in)

    def means_along():
        for s, k in x_first:
            along_z(s, k).wait_recv()
            mean(s, k, dn_z, up_z)

    when_not(gets_on, means_near)
    when(gets_on, means_along)
    for s, k in Z_FIRST:
        away(s, k).wait_recv()
        mean(s, k, dn_in, up_in)

    for kind in range(2):
        for i in range(CHUNKS):
            far(kind, i).wait_send()
            relay(kind, i).wait_send()
        for b in range(own_blocks):
            near(kind, b).wait_send()
    for s in range(SLICES):
        for o in range(3):
            weights(s, o).wait_send()
            grads(s, o).wait_send()
    for s, k in pieces:
        away(s, k).wait_send()

    def sent_along(some):
        for s, k in some:
            along_z(s, k).wait_send()

    when(gets_on, partial(sent_along, x_first))
    when(sends_on, partial(sent_along, Z_FIRST))


def flush_kernel(*refs):
    held, out, sem = refs[:6], refs[6:12], refs[12]
    copies = [pltpu.make_async_copy(held[i], out[i], sem.at[i]) for i in range(6)]
    for copy in copies:
        copy.start()
    for copy in copies:
        copy.wait()


def flush(*arrays):
    return pl.pallas_call(
        flush_kernel,
        out_shape=[jax.ShapeDtypeStruct(a.shape, a.dtype) for a in arrays],
        in_specs=[pl.BlockSpec(memory_space=pl.ANY)] * 6,
        out_specs=[pl.BlockSpec(memory_space=pl.ANY)] * 6,
        scratch_shapes=[pltpu.SemaphoreType.DMA((6,))],
        compiler_params=pltpu.CompilerParams(vmem_limit_bytes=4 * 1024 * 1024),
        name="flush",
    )(*arrays)


def fused(level, peers, fix, *arrays):
    tokens, out_grad, up_param, down_param = arrays[:4]
    rows, width = tokens.shape
    hid = down_param.shape[0]
    part, full = up_param.shape
    span = hid // SLICES
    piece = rows // CHUNKS
    block = 2 * piece
    blocks = 4 * rows // block
    own_blocks = rows // block
    dma = pltpu.SemaphoreType.DMA
    vmem = pltpu.VMEM
    shapes = [
        pltpu.VMEM(up_param.shape, F32),
        pltpu.VMEM(down_param.shape, F32),
    ] * 3
    return pl.pallas_call(
        partial(kernel, peers, 2**level),
        out_shape=shapes,
        in_specs=[pl.BlockSpec(memory_space=pltpu.SMEM)] + [pl.BlockSpec(memory_space=pl.ANY)] * 8,
        out_specs=[pl.BlockSpec(memory_space=pltpu.VMEM)] * 6,
        scratch_shapes=[
            vmem((blocks, block, width), BF16),
            vmem((blocks, block, width), BF16),
            vmem((blocks, block, width), BF16),
            vmem((SLICES, 4, part, span), BF16),
            vmem((SLICES, 4, part, span), BF16),
            vmem((span, width), BF16),
            vmem((hid, width), BF16),
            vmem((span, block), BF16),
            vmem((span, block), F32),
            vmem((span, width), F32),
            vmem((span, width), F32),
            vmem((SLICES, 4, part, span), BF16),
            vmem((SLICES, 4, part, span), BF16),
            vmem((SLICES, span, width), BF16),
            vmem((SLICES, span, width), BF16),
            vmem((SLICES, 4, part, span), BF16),
            vmem((SLICES, 4, part, span), BF16),
            vmem((SLICES, span, width), BF16),
            vmem((SLICES, 4, part, span), BF16),
            dma((6 + 2 * own_blocks,)),
            dma((2, CHUNKS)),
            dma((2, CHUNKS)),
            dma((2, CHUNKS)),
            dma((2, CHUNKS)),
            dma((2, own_blocks)),
            dma((2, own_blocks)),
            dma((SLICES, 3)),
            dma((SLICES, 3)),
            dma((SLICES, 3)),
            dma((SLICES, 3)),
            dma((SLICES, 4)),
            dma((SLICES, 4)),
            dma((SLICES, 4)),
            dma((SLICES, 4)),
        ],
        compiler_params=pltpu.CompilerParams(
            collective_id=level, has_side_effects=True, vmem_limit_bytes=46 * 1024 * 1024
        ),
        name="adam_step",
    )(fix, *arrays)


def step_at(level, peers, fix, *arrays):
    return flush(*fused(level, peers, fix, *arrays))


def body(
    tokens, out_grad, step, up_param, down_param, up_first, down_first, up_second, down_second
):
    peers = lax.axis_size("peer")
    count = (step[0] + 1).astype(F32)
    first_fix = 1.0 - jnp.power(F32(0.9), count)
    second_fix = 1.0 - jnp.power(F32(0.999), count)
    fix = jnp.stack([0.01 / first_fix, 1.0 / second_fix])
    levels = peers.bit_length() - 1
    arrays = [
        a[0]
        for a in (
            tokens, out_grad, up_param, down_param, up_first, down_first, up_second, down_second
        )
    ]
    branches = [partial(step_at, level, peers) for level in range(levels)]
    outs = lax.switch(step[0] % levels, branches, fix, *arrays)
    return tuple(o[None] for o in outs)


def solution(mesh):
    sharded = P("peer", "zero", None)
    return jax.shard_map(
        body,
        mesh=mesh,
        in_specs=(sharded, sharded, P()) + (sharded,) * 6,
        out_specs=(sharded,) * 6,
        check_vma=False,
    )
```

```python
from functools import partial

import jax
import jax.numpy as jnp
from jax import lax
from jax.experimental import pallas as pl
from jax.experimental.pallas import tpu as pltpu
from jax.sharding import PartitionSpec as P

MESH = pl.DeviceIdType.MESH
SLICES = 4
CHUNKS = 4
Z_FIRST = ((1, 2), (1, 3), (3, 0), (3, 1), (3, 2), (3, 3))
ON_LOOP = {1: ((0, 0), (0, 1))}
ON_AFTER = {2: ((0, 2), (0, 3)), 3: ((1, 0), (1, 1), (2, 0), (2, 1))}
ON_LAST = ((2, 2), (2, 3))
GO_LOOP = {3: ((1, 2), (1, 3))}
GO_LAST = ((3, 0), (3, 1), (3, 2), (3, 3))
BF16 = jnp.bfloat16
F32 = jnp.float32


def dot(left, right, dims):
    return lax.dot_general(left, right, (dims, ((), ())), preferred_element_type=F32)


def kernel(
    peers,
    distance,
    fix,
    tokens,
    out_grad,
    up_param,
    down_param,
    up_first,
    down_first,
    up_second,
    down_second,
    up_p,
    dn_p,
    up_f,
    dn_f,
    up_s,
    dn_s,
    tok,
    grd,
    nrm,
    upw_send,
    upw,
    up_t,
    down_low,
    act,
    slope,
    acc_up,
    acc_down,
    ug_send,
    ug,
    dn_out,
    dn_in,
    up_out,
    up_in,
    dn_z,
    up_z,
    load_sem,
    far_send,
    far_recv,
    relay_send,
    relay_recv,
    near_send,
    near_recv,
    upw_ssem,
    upw_rsem,
    ug_ssem,
    ug_rsem,
    away_ssem,
    away_rsem,
    z_ssem,
    z_rsem,
):
    rows, width = tokens.shape
    hid = down_param.shape[0]
    part = up_param.shape[0]
    span = hid // SLICES
    piece = rows // CHUNKS
    block = 2 * piece
    own_blocks = rows // block
    blocks = tok.shape[0]
    near_blocks = 2 * own_blocks

    peer = lax.axis_index("peer")
    me = lax.axis_index("zero")
    mate = me + 1 - 2 * (me % 2)
    cross = (me + 2) % 4
    diagonal = 3 - me
    group = (cross, diagonal, mate)
    half = peers // 2
    twin = (peer + half) % peers
    if distance < half:
        upper = peer // half
        place = peer % half
        sends_on = place < distance
        gets_on = place + distance >= half
        onto = upper * half + (place + half - distance) % half
        source = upper * half + (place + distance) % half
    else:
        sends_on = gets_on = None
        onto = source = twin

    def local(src, dst, sem):
        return pltpu.make_async_copy(src, dst, sem)

    def remote(src, dst, ssem, rsem, **where):
        return pltpu.make_async_remote_copy(
            src_ref=src, dst_ref=dst, send_sem=ssem, recv_sem=rsem, device_id=where, device_id_type=MESH
        )

    loads = [
        local(up_param, up_p, load_sem.at[0]),
        local(down_param, dn_p, load_sem.at[1]),
        local(down_first, dn_f, load_sem.at[2]),
        local(down_second, dn_s, load_sem.at[3]),
        local(up_first, up_f, load_sem.at[4]),
        local(up_second, up_s, load_sem.at[5]),
    ]
    for b in range(own_blocks):
        at = pl.ds(b * block, block)
        loads.append(local(tokens.at[at], tok.at[b], load_sem.at[6 + 2 * b]))
        loads.append(local(out_grad.at[at], grd.at[b], load_sem.at[7 + 2 * b]))
    loads[0].start()

    barrier = pltpu.get_barrier_semaphore()
    for other in group:
        pl.semaphore_signal(barrier, inc=1, device_id={"zero": other}, device_id_type=MESH)
    others = (onto, source) if sends_on is None else (onto, source, twin)
    for other in others:
        pl.semaphore_signal(barrier, inc=1, device_id={"peer": other}, device_id_type=MESH)
    for copy in loads[1:]:
        copy.start()

    def far(kind, i):
        src, dst = ((tokens, tok), (out_grad, grd))[kind]
        at = pl.ds(pl.multiple_of(i * piece, piece), piece)
        return remote(
            src.at[at],
            dst.at[near_blocks + i, pl.ds(0, piece)],
            far_send.at[kind, i],
            far_recv.at[kind, i],
            zero=cross,
        )

    def relay(kind, i):
        dst = (tok, grd)[kind]
        return remote(
            dst.at[near_blocks + i, pl.ds(0, piece)],
            dst.at[near_blocks + i, pl.ds(piece, piece)],
            relay_send.at[kind, i],
            relay_recv.at[kind, i],
            zero=mate,
        )

    def near(kind, b):
        src, dst = ((tokens, tok), (out_grad, grd))[kind]
        return remote(
            src.at[pl.ds(b * block, block)],
            dst.at[own_blocks + b],
            near_send.at[kind, b],
            near_recv.at[kind, b],
            zero=mate,
        )

    def weights(s, o):
        return remote(
            upw_send.at[s, group[o]], upw.at[s, me], upw_ssem.at[s, o], upw_rsem.at[s, o], zero=group[o]
        )

    def weights_in(s, o):
        return remote(
            upw_send.at[s, group[o]], upw.at[s, group[o]], upw_ssem.at[s, o], upw_rsem.at[s, o], zero=group[o]
        )

    def grads(s, o):
        return remote(ug_send.at[s, group[o]], ug.at[s, me], ug_ssem.at[s, o], ug_rsem.at[s, o], zero=group[o])

    def grads_in(s, o):
        return remote(
            ug_send.at[s, group[o]], ug.at[s, group[o]], ug_ssem.at[s, o], ug_rsem.at[s, o], zero=group[o]
        )

    def cut(s, k):
        if k < 2:
            at = pl.ds(k * (span // 2), span // 2)
            return [ref.at[s, at] for ref in (dn_out, dn_in, dn_z)]
        at = pl.ds(2 * (k - 2), 2)
        return [ref.at[s, at] for ref in (up_out, up_in, up_z)]

    def away(s, k):
        out, into, _ = cut(s, k)
        return remote(out, into, away_ssem.at[s, k], away_rsem.at[s, k], peer=onto)

    def away_later(s, k):
        _, into, along = cut(s, k)
        return remote(along, into, away_ssem.at[s, k], away_rsem.at[s, k], peer=onto)

    def along_z(s, k):
        out, into, along = cut(s, k)
        return remote(out if (s, k) in Z_FIRST else into, along, z_ssem.at[s, k], z_rsem.at[s, k], peer=twin)

    def when(flag, run):
        if flag is not None:
            pl.when(flag)(run)

    def when_not(flag, run):
        if flag is None:
            run()
        else:
            pl.when(jnp.logical_not(flag))(run)

    pl.semaphore_wait(barrier, len(group) + len(others))
    far(0, 0).start()
    for kind in range(2):
        for b in range(own_blocks):
            near(kind, b).start()

    loads[0].wait()
    for s in range(SLICES):

        def lower(j, carry):
            at = pl.ds(pl.multiple_of(j * hid + s * span, span), span)
            upw_send[s, j] = up_p[:, at].astype(BF16)
            return carry

        lax.fori_loop(0, 4, lower, 0)
    for o in range(3):
        weights(0, o).start()
    far(1, 0).start()
    for i in range(1, CHUNKS):
        far(0, i).start()
        far(1, i).start()
    for o in range(3):
        weights(1, o).start()

    for s in range(SLICES):
        upw[s, me] = upw_send[s, me]
    loads[1].wait()

    def lower_down(r, carry):
        at = pl.ds(pl.multiple_of(r * (hid // 8), hid // 8), hid // 8)
        down_low[at] = dn_p[at].astype(BF16)
        return carry

    lax.fori_loop(0, 8, lower_down, 0)
    for copy in loads[6:]:
        copy.wait()

    def arrange(s):
        for o in range(3):
            weights_in(s, o).wait_recv()

        def turn(j, carry):
            up_t[:, pl.ds(pl.multiple_of(j * part, part), part)] = upw[s, j].astype(F32).T.astype(BF16)
            return carry

        lax.fori_loop(0, 4, turn, 0)

    def forward(b):
        pre = dot(up_t[...], nrm[b], ((1,), (1,)))
        cube = 0.044715 * pre * pre
        t = jnp.tanh(0.7978845608 * (pre + cube * pre))
        half = 0.5 * (1.0 + t)
        act[...] = (pre * half).astype(BF16)
        slope[...] = half + 0.5 * pre * (1.0 - t * t) * (0.7978845608 * (1.0 + 3.0 * cube))

    def gradients(s, b):
        act_grad = dot(down_low[pl.ds(s * span, span)], grd[b], ((1,), (1,)))
        pre_grad = (act_grad * slope[...]).astype(BF16)
        down = dot(act[...], grd[b], ((1,), (0,)))
        up = dot(pre_grad, nrm[b], ((1,), (0,)))
        acc_down[...] += down
        acc_up[...] += up

    def clear():
        acc_down[...] = jnp.zeros_like(acc_down)
        acc_up[...] = jnp.zeros_like(acc_up)

    def normalise(b):
        step = block // 4

        def some(r, carry):
            at = pl.ds(pl.multiple_of(r * step, step), step)
            wide = tok[b, at].astype(F32)
            center = jnp.mean(wide, axis=1, keepdims=True)
            wide = wide - center
            spread = jnp.mean(wide * wide, axis=1, keepdims=True)
            nrm[b, at] = (wide * lax.rsqrt(spread + 1e-05)).astype(BF16)
            return carry

        lax.fori_loop(0, 4, some, 0)

    def adam(param, first, second, grad):
        first_new = 0.9 * first + 0.1 * grad
        second_new = 0.999 * second + 0.001 * grad * grad
        step = (fix[0] * first_new) / (jnp.sqrt(second_new * fix[1]) + 1e-08)
        return param - step, first_new, second_new

    def down_update(s):
        tall = span // 2

        def some(r, carry):
            here = pl.ds(pl.multiple_of(r * tall, tall), tall)
            at = pl.ds(pl.multiple_of(s * span + r * tall, tall), tall)
            fresh = adam(dn_p[at], dn_f[at], dn_s[at], acc_down[here])
            dn_p[at], dn_f[at], dn_s[at] = fresh
            dn_out[s, here] = fresh[0].astype(BF16)
            return carry

        lax.fori_loop(0, 2, some, 0)

    def up_update(s):
        def some(j, carry):
            at = pl.ds(pl.multiple_of(j * hid + s * span, span), span)
            fresh = adam(up_p[:, at], up_f[:, at], up_s[:, at], ug[s, j].astype(F32))
            up_p[:, at], up_f[:, at], up_s[:, at] = fresh
            up_out[s, j] = fresh[0].astype(BF16)
            return carry

        lax.fori_loop(0, 4, some, 0)

    def share(s):
        def turn(j, carry):
            at = pl.ds(pl.multiple_of(j * part, part), part)
            ug_send[s, j] = acc_up[:, at].T.astype(BF16)
            return carry

        lax.fori_loop(0, 4, turn, 0)

    clear()
    arrange(0)

    def first_pass(b, carry):
        i = jnp.maximum(b - near_blocks, 0)

        @pl.when(jnp.logical_and(b >= own_blocks, b < near_blocks))
        def _():
            remote_near(0, b).wait_recv()

        @pl.when(b >= near_blocks)
        def _():
            far(0, i).wait_recv()
            relay(0, i).start()
            relay(0, i).wait_recv()

        normalise(b)
        forward(b)

        @pl.when(jnp.logical_and(b >= own_blocks, b < near_blocks))
        def _():
            remote_near(1, b).wait_recv()

        @pl.when(b >= near_blocks)
        def _():
            far(1, i).wait_recv()
            relay(1, i).start()
            relay(1, i).wait_recv()

        gradients(0, b)
        return carry

    def remote_near(kind, b):
        src, dst = ((tokens, tok), (out_grad, grd))[kind]
        n = jnp.clip(b - own_blocks, 0, own_blocks - 1)
        return remote(
            src.at[pl.ds(pl.multiple_of(n * block, block), block)],
            dst.at[own_blocks + n],
            near_send.at[kind, n],
            near_recv.at[kind, n],
            zero=mate,
        )

    lax.fori_loop(0, blocks, first_pass, 0)

    for copy in loads[2:6]:
        copy.wait()

    def depart(s, k):
        if (s, k) in Z_FIRST:
            when_not(sends_on, lambda: away(s, k).start())
            if sends_on is not None:
                when(sends_on, lambda: along_z(s, k).start())
        else:
            away(s, k).start()

    def pass_on(pieces):
        def run():
            for s, k in pieces:
                away(s, k).wait_recv()
                along_z(s, k).start()

        if pieces:
            when(gets_on, run)

    def go_on(pieces):
        def run():
            for s, k in pieces:
                along_z(s, k).wait_recv()
                away_later(s, k).start()

        if pieces:
            when(sends_on, run)

    def exchange(s):
        ug[s, me] = ug_send[s, me]
        for o in range(3):
            grads(s, o).start()
        if s + 2 < SLICES:
            for o in range(3):
                weights(s + 2, o).start()

    def finish(s):
        share(s)
        exchange(s)
        down_update(s)
        depart(s, 0)
        depart(s, 1)

    def finish_up(s):
        for o in range(3):
            grads_in(s, o).wait_recv()
        up_update(s)
        depart(s, 2)
        depart(s, 3)

    finish(0)

    for s in range(1, SLICES):
        clear()
        arrange(s)

        def pass_over(b, carry, s=s):
            @pl.when(b == (blocks - 3 if s == 1 else blocks - 2))
            def _():
                finish_up(s - 1)

            if s in ON_LOOP or s in GO_LOOP:

                @pl.when(b == blocks - 1)
                def _():
                    pass_on(ON_LOOP.get(s))
                    go_on(GO_LOOP.get(s))

            forward(b)
            gradients(s, b)
            return carry

        lax.fori_loop(0, blocks, pass_over, 0)
        finish(s)
        pass_on(ON_AFTER.get(s))
    finish_up(SLICES - 1)
    pass_on(ON_LAST)

    go_on(GO_LAST)

    def mean(s, k, down, up):
        if k < 2:
            tall = span // 8

            def rows_mean(r, carry):
                r = r + 4 * k
                here = pl.ds(pl.multiple_of(r * tall, tall), tall)
                at = pl.ds(pl.multiple_of(s * span + r * tall, tall), tall)
                dn_p[at] = 0.5 * (dn_p[at] + down[s, here].astype(F32))
                return carry

            lax.fori_loop(0, 4, rows_mean, 0)
        else:
            tall = part // 4

            def columns_mean(n, carry):
                j = 2 * k - 4 + n // 4
                here = pl.ds(pl.multiple_of(n % 4 * tall, tall), tall)
                at = pl.ds(pl.multiple_of(j * hid + s * span, span), span)
                up_p[here, at] = 0.5 * (up_p[here, at] + up[s, j, here].astype(F32))
                return carry

            lax.fori_loop(0, 8, columns_mean, 0)

    pieces = [(s, k) for s in range(SLICES) for k in range(4)]
    x_first = [piece for piece in pieces if piece not in Z_FIRST]

    def means_near():
        for s, k in x_first:
            away(s, k).wait_recv()
            mean(s, k, dn_in, up_in)

    def means_along():
        for s, k in x_first:
            along_z(s, k).wait_recv()
            mean(s, k, dn_z, up_z)

    when_not(gets_on, means_near)
    when(gets_on, means_along)
    for s, k in Z_FIRST:
        away(s, k).wait_recv()
        mean(s, k, dn_in, up_in)

    for kind in range(2):
        for i in range(CHUNKS):
            far(kind, i).wait_send()
            relay(kind, i).wait_send()
        for b in range(own_blocks):
            near(kind, b).wait_send()
    for s in range(SLICES):
        for o in range(3):
            weights(s, o).wait_send()
            grads(s, o).wait_send()
    for s, k in pieces:
        away(s, k).wait_send()

    def sent_along(some):
        for s, k in some:
            along_z(s, k).wait_send()

    when(gets_on, partial(sent_along, x_first))
    when(sends_on, partial(sent_along, Z_FIRST))


def flush_kernel(*refs):
    held, out, sem = refs[:6], refs[6:12], refs[12]
    copies = [pltpu.make_async_copy(held[i], out[i], sem.at[i]) for i in range(6)]
    for copy in copies:
        copy.start()
    for copy in copies:
        copy.wait()


def flush(*arrays):
    return pl.pallas_call(
        flush_kernel,
        out_shape=[jax.ShapeDtypeStruct(a.shape, a.dtype) for a in arrays],
        in_specs=[pl.BlockSpec(memory_space=pl.ANY)] * 6,
        out_specs=[pl.BlockSpec(memory_space=pl.ANY)] * 6,
        scratch_shapes=[pltpu.SemaphoreType.DMA((6,))],
        compiler_params=pltpu.CompilerParams(vmem_limit_bytes=4 * 1024 * 1024),
        name="flush",
    )(*arrays)


def fused(level, peers, fix, *arrays):
    tokens, out_grad, up_param, down_param = arrays[:4]
    rows, width = tokens.shape
    hid = down_param.shape[0]
    part, full = up_param.shape
    span = hid // SLICES
    piece = rows // CHUNKS
    block = 2 * piece
    blocks = 4 * rows // block
    own_blocks = rows // block
    dma = pltpu.SemaphoreType.DMA
    vmem = pltpu.VMEM
    shapes = [
        pltpu.VMEM(up_param.shape, F32),
        pltpu.VMEM(down_param.shape, F32),
    ] * 3
    return pl.pallas_call(
        partial(kernel, peers, 2**level),
        out_shape=shapes,
        in_specs=[pl.BlockSpec(memory_space=pltpu.SMEM)] + [pl.BlockSpec(memory_space=pl.ANY)] * 8,
        out_specs=[pl.BlockSpec(memory_space=pltpu.VMEM)] * 6,
        scratch_shapes=[
            vmem((blocks, block, width), BF16),
            vmem((blocks, block, width), BF16),
            vmem((blocks, block, width), BF16),
            vmem((SLICES, 4, part, span), BF16),
            vmem((SLICES, 4, part, span), BF16),
            vmem((span, width), BF16),
            vmem((hid, width), BF16),
            vmem((span, block), BF16),
            vmem((span, block), F32),
            vmem((span, width), F32),
            vmem((span, width), F32),
            vmem((SLICES, 4, part, span), BF16),
            vmem((SLICES, 4, part, span), BF16),
            vmem((SLICES, span, width), BF16),
            vmem((SLICES, span, width), BF16),
            vmem((SLICES, 4, part, span), BF16),
            vmem((SLICES, 4, part, span), BF16),
            vmem((SLICES, span, width), BF16),
            vmem((SLICES, 4, part, span), BF16),
            dma((6 + 2 * own_blocks,)),
            dma((2, CHUNKS)),
            dma((2, CHUNKS)),
            dma((2, CHUNKS)),
            dma((2, CHUNKS)),
            dma((2, own_blocks)),
            dma((2, own_blocks)),
            dma((SLICES, 3)),
            dma((SLICES, 3)),
            dma((SLICES, 3)),
            dma((SLICES, 3)),
            dma((SLICES, 4)),
            dma((SLICES, 4)),
            dma((SLICES, 4)),
            dma((SLICES, 4)),
        ],
        compiler_params=pltpu.CompilerParams(
            collective_id=level, has_side_effects=True, vmem_limit_bytes=46 * 1024 * 1024
        ),
        name="adam_step",
    )(fix, *arrays)


def step_at(level, peers, fix, *arrays):
    return flush(*fused(level, peers, fix, *arrays))


def body(
    tokens, out_grad, step, up_param, down_param, up_first, down_first, up_second, down_second
):
    peers = lax.axis_size("peer")
    count = (step[0] + 1).astype(F32)
    first_fix = 1.0 - jnp.power(F32(0.9), count)
    second_fix = 1.0 - jnp.power(F32(0.999), count)
    fix = jnp.stack([0.01 / first_fix, 1.0 / second_fix])
    levels = peers.bit_length() - 1
    arrays = [
        a[0]
        for a in (
            tokens, out_grad, up_param, down_param, up_first, down_first, up_second, down_second
        )
    ]
    branches = [partial(step_at, level, peers) for level in range(levels)]
    outs = lax.switch(step[0] % levels, branches, fix, *arrays)
    return tuple(o[None] for o in outs)


def solution(mesh):
    sharded = P("peer", "zero", None)
    return jax.shard_map(
        body,
        mesh=mesh,
        in_specs=(sharded, sharded, P()) + (sharded,) * 6,
        out_specs=(sharded,) * 6,
        check_vma=False,
    )
```
